32 devices in a mesh: member: 2 (over y), lat: 16 (over z, x, core).
Axes of the slice: x: 2, y: 2, z: 4, core: 2. Of those that a mesh axis runs over, the one named last changes fastest.
Arguments:
- tracers: float32 [60, 4, 64, 1440], P('member', None, 'lat'), parts along dimension 0, may hold values from -6 to 6
- currents: float32 [4, 4, 64, 1440], P('member', None, 'lat'), parts along dimension 0, may hold values from -0.4 to 0.4
- column_levels: int32 [128, 1440], P(('member', 'lat')), parts along dimension 0, may hold values from 0 to 4
Outputs:
- advected: float32 [60, 4, 64, 1440], P('member', None, 'lat'), parts along dimension 0
The draws below stay inside these ranges and needn't reach their ends.
There are 2 independent parts, one for each index of `member`. The reference program is written for one: setup_inputs(seed, part) draws one part's arguments, and reference() takes and returns one part's arrays. A program takes and returns all parts, laid end to end along the dimension named above; each array names one. Nothing has to cross between parts.
All inputs are finite; a program needn't handle non-finite values.
Results may differ from the reference program's by a relative error of at most 0.00002.
Values sent between devices are 32-bit elements; how exact they have to be, the bound alone decides.
A program may use at most 64 MiB of HBM per device.

```python
import jax
import jax.numpy as jnp

TRACERS = 30
LEVELS = 4
NLON = 1440
NLAT = 64


def place_ends(values, own_key, least, top_value):
    longest = values.shape.index(max(values.shape))
    spots = []
    for shift in (0, 1):
        where = [jax.random.randint(jax.random.fold_in(own_key, axis), (), 0, length) for axis, length in enumerate(values.shape)]
        where[longest] = (where[longest] + shift) % values.shape[longest]
        spots.append(tuple(where))
    return values.at[spots[0]].set(least).at[spots[1]].set(top_value)


def shard_levels(rng, shape, shards, least, high):
    level, own = 1.0, jax.random.fold_in(rng, 6)
    for position, parts in shards:
        steps = jnp.exp(jax.random.uniform(jax.random.fold_in(own, position), (parts,), jnp.float32, least / len(shards), high / len(shards)))
        level = level * jnp.repeat(steps, shape[position] // parts).reshape([-1 if axis == position else 1 for axis in range(len(shape))])
    return level


def scatter_about(rng, dims, spread, limit, pieces=(), kind=jnp.bfloat16):
    gain = shard_levels(rng, dims, pieces, -0.22, 0.18) if pieces else 1.0
    result = jax.random.normal(rng, dims, jnp.float32) * spread * gain
    return jnp.minimum(jnp.maximum(result, -limit), limit).astype(kind)


def setup_inputs(seed: int = 0, part: int = 0) -> dict:
    splits = jax.random.split(jax.random.key(seed), 4)
    part_splits = jax.random.split(jax.random.fold_in(splits[3], part), 4)
    tracers = scatter_about(part_splits[0], (TRACERS, LEVELS, NLAT, NLON), 1.0, 6.0, ((2, 16),), jnp.float32)
    currents = jnp.clip(jax.random.uniform(part_splits[1], (2, LEVELS, NLAT, NLON), jnp.float32, -0.4, 0.4) * shard_levels(part_splits[1], (2, LEVELS, NLAT, NLON), ((2, 16),), -0.4, 0.0), -0.4, 0.4)
    column_levels = place_ends(jax.random.randint(part_splits[2], (NLAT, NLON), 0, LEVELS + 1), jax.random.fold_in(part_splits[2], 1), 0, LEVELS).astype(jnp.int32)
    return {"tracers": tracers, "currents": currents, "column_levels": column_levels}


def face_flux(courant, before, left, right, after):
    central = courant * (7.0 * (left + right) - (before + after)) / 12.0
    upwind = jnp.abs(courant) * (3.0 * (right - left) - (after - before)) / 12.0
    return central - upwind


def advect_section(padded, east_pad, north_pad, wet_pad):
    rows = padded.shape[-2] - 4
    field = padded[..., 2:-2, :]
    east = east_pad[:, 1:-1]
    wet_rows = wet_pad[:, 1:-1]
    east_face = 0.5 * (east + jnp.roll(east, -1, -1))
    east_open = wet_rows * jnp.roll(wet_rows, -1, -1)
    east_flux = east_open * face_flux(east_face, jnp.roll(field, 1, -1), field, jnp.roll(field, -1, -1), jnp.roll(field, -2, -1))
    east_div = east_flux - jnp.roll(east_flux, 1, -1)
    north_face = 0.5 * (north_pad[:, :-1] + north_pad[:, 1:])
    north_open = wet_pad[:, :-1] * wet_pad[:, 1:]
    north_flux = north_open * face_flux(north_face, padded[..., 0:rows + 1, :], padded[..., 1:rows + 2, :], padded[..., 2:rows + 3, :], padded[..., 3:rows + 4, :])
    north_div = north_flux[..., 1:, :] - north_flux[..., :-1, :]
    return field - east_div - north_div


def extend(field, width, factor):
    south = jnp.zeros(field.shape[:-2] + (width, field.shape[-1]), jnp.float32)
    north = factor * jnp.flip(field[..., field.shape[-2] - width:, :], axis=(-2, -1))
    return jnp.concatenate([south, field, north], axis=-2)


def reference(tracers, currents, column_levels):
    levels = jnp.arange(tracers.shape[1], dtype=jnp.int32)
    wet = (levels[:, None, None] < column_levels[None]).astype(jnp.float32)
    east_pad = extend(currents[0], 1, -1.0)
    north_pad = extend(currents[1], 1, -1.0)
    wet_pad = extend(wet, 1, 1.0)
    start = tracers * wet
    first = advect_section(extend(start, 2, 1.0), east_pad, north_pad, wet_pad) * wet
    second = advect_section(extend(first, 2, 1.0), east_pad, north_pad, wet_pad)
    return 0.5 * (start + second) * wet
```

```python
import functools

import jax
import jax.numpy as jnp
from jax import lax
from jax.experimental import pallas as pl
from jax.experimental.pallas import tpu as pltpu
from jax.sharding import PartitionSpec as P

LANES = 128
SUB = 8
WRAP = 4
HALO = 2
MESH = pl.DeviceIdType.MESH


def wrapped(x, nlon):
    rest = nlon % LANES
    whole = nlon - rest
    tail = jnp.concatenate([x[:, whole:], x[:, : LANES - rest]], axis=1)
    lane = lax.broadcasted_iota(jnp.int32, tail.shape, 1)
    tail = jnp.where(lane >= LANES - WRAP, pltpu.roll(tail, LANES - rest, 1), tail)
    return jnp.concatenate([x[:, :whole], tail], axis=1)


def joined(main, tail, rest):
    lane = lax.broadcasted_iota(jnp.int32, tail.shape, 1)
    west = pltpu.roll(tail, LANES - rest, 1)
    tail = jnp.where(lane < rest, tail, pltpu.roll(main[:, :LANES], rest, 1))
    tail = jnp.where(lane >= LANES - WRAP, west, tail)
    return jnp.concatenate([main, tail], axis=1)


def packed(a, b, rest):
    lane = lax.broadcasted_iota(jnp.int32, a.shape, 1)
    both = jnp.where(lane < rest, a, pltpu.roll(b, rest, 1))
    other = pltpu.roll(pltpu.roll(both, SUB // 2, 0), LANES // 2, 1)
    return jnp.where(lane < LANES // 2, both, other)[: SUB // 2]


def unpacked(half, rest):
    x = jnp.concatenate([half, half], axis=0)
    row = lax.broadcasted_iota(jnp.int32, x.shape, 0)
    x = jnp.where(row < SUB // 2, x, pltpu.roll(x, LANES // 2, 1))
    return x, pltpu.roll(x, LANES - rest, 1)


def face_terms(c, opened):
    c = c * opened * (1.0 / 12.0)
    m = jnp.abs(c)
    return -c - m, 7.0 * c + 3.0 * m, 7.0 * c - 3.0 * m, m - c


def mirrored(tiles, nlon):
    count = len(tiles)
    rest = nlon % LANES
    row = lax.broadcasted_iota(jnp.int32, (LANES, LANES), 0)
    col = lax.broadcasted_iota(jnp.int32, (LANES, LANES), 1)
    near = jnp.where((row + col == rest - 1), 1.0, 0.0).astype(jnp.float32)
    far = jnp.where((row + col == LANES + rest - 1), 1.0, 0.0).astype(jnp.float32)
    dot = functools.partial(
        jnp.dot, precision=lax.Precision.HIGHEST, preferred_element_type=jnp.float32
    )
    return [
        dot(tiles[(count - 1 - q) % count], near) + dot(tiles[(count - 2 - q) % count], far)
        for q in range(count)
    ]


def kernel(
    nlon, levels, group, raw_hbm, flow_hbm, lev_hbm, out_ref,
    raw, raw_flow, lev_ref, start, first, partial, lo, hi, relay, pack_up, pack_dn, pack_lo, pack_hi,
    flow, v_lo, v_hi, lev_up, lev_dn, lev_lo, lev_hi, coef, edge, wets, halo,
    load, aux_load, send_up, send_dn, recv_lo, recv_hi, relay_in, relay_out,
    psend_up, psend_dn, precv_lo, precv_hi, fsend, frecv,
):
    lat = lax.axis_size("lat")
    me = lax.axis_index("lat")
    rows, planes, width = start.shape
    rest = nlon % LANES
    whole = nlon - rest
    chunks = planes // SUB
    layers = lat // group
    layer = me // group
    place = me % group
    relays = layers > 1 and group > 2 and lat % group == 0
    has_lo = me > 0
    has_hi = me < lat - 1
    is_first = place == 0
    is_last = place == group - 1
    barrier = pltpu.get_barrier_semaphore()

    pairs = [(has_lo, -1), (has_hi, 1)]
    if relays:
        pairs += [
            (is_first, group - 1),
            (is_last, 1 - group),
            ((is_first | is_last) & (layer < layers - 1), group),
            ((is_first | is_last) & (layer > 0), -group),
        ]

    def part_of(g):
        return pl.ds(pl.multiple_of(g * SUB, SUB), SUB)

    def loading(g):
        part = part_of(g)
        return pltpu.make_async_copy(raw_hbm.at[part], raw.at[part], load.at[g])

    lev_load = pltpu.make_async_copy(lev_hbm, lev_ref, aux_load.at[0])
    flow_load = pltpu.make_async_copy(flow_hbm, raw_flow, aux_load.at[1])
    lev_load.start()
    loading(0).start()
    flow_load.start()

    for near, by in pairs:
        @pl.when(near)
        def _(by=by):
            pl.semaphore_signal(barrier, inc=1, device_id={"lat": me + by}, device_id_type=MESH)

    def load_rest(g, carry):
        loading(g).start()
        return carry

    lax.fori_loop(1, chunks, load_rest, 0)

    ranks = lax.rem(lax.broadcasted_iota(jnp.int32, (SUB, nlon), 0), levels)

    def wet_of(row):
        lev = jnp.broadcast_to(row, (SUB, nlon))
        return wrapped(jnp.where(ranks < lev, 1.0, 0.0), nlon)

    lev_load.wait()
    for k in range(rows):
        wets[k + 1] = wet_of(lev_ref[k : k + 1, :])
    lev_up[...] = lev_ref[rows - 1 : rows, :]
    lev_dn[...] = lev_ref[0:1, :]

    def put_packs(phase, g, tail):
        pack_up[phase, g] = packed(tail(rows - 2), tail(rows - 1), rest)
        pack_dn[phase, g] = packed(tail(0), tail(1), rest)

    def reorder(g):
        part = part_of(g)
        loading(g).wait()
        tails = []
        for k in range(rows):
            x = wrapped(raw[part, k, :], nlon) * wets[k + 1]
            start[k, part, :] = x
            tails.append(x[:, whole:])
        put_packs(0, g, lambda k: tails[k])

    reorder(0)
    flow_load.wait()
    for k in range(rows):
        for which in range(2):
            flow[which, k] = raw_flow[which, :, k, :]

    pl.semaphore_wait(barrier, sum(jnp.where(near, 1, 0) for near, _ in pairs))

    def remote(src, dst, s, r, by):
        return pltpu.make_async_remote_copy(
            src_ref=src, dst_ref=dst, send_sem=s, recv_sem=r,
            device_id={"lat": me + by}, device_id_type=MESH,
        )

    def flows(up):
        n = 0 if up else 2
        if up:
            pieces = [(flow.at[1, rows - 1], v_lo), (lev_up, lev_lo)]
        else:
            pieces = [(flow.at[1, 0], v_hi), (lev_dn, lev_hi)]
        by = 1 if up else -1
        return [
            remote(src, dst, fsend.at[n + i], frecv.at[n + i], by)
            for i, (src, dst) in enumerate(pieces)
        ]

    def main(phase, up, g, via):
        part = part_of(g)
        own = first if phase else start
        src = own.at[pl.ds(rows - HALO if up else 0, HALO), part, pl.ds(0, whole)]
        s = (send_up if up else send_dn).at[phase, g]
        if via:
            by = 1 - group if up else group - 1
            return remote(src, relay.at[phase, :, part], s, relay_in.at[phase, g], by)
        dst = (lo if up else hi).at[phase, :, part]
        r = (recv_lo if up else recv_hi).at[phase, g]
        return remote(src, dst, s, r, 1 if up else -1)

    def tails(phase, up, g):
        if up:
            return remote(pack_up.at[phase, g], pack_lo.at[phase, g],
                          psend_up.at[phase, g], precv_lo.at[phase, g], 1)
        return remote(pack_dn.at[phase, g], pack_hi.at[phase, g],
                      psend_dn.at[phase, g], precv_hi.at[phase, g], -1)

    def forward(phase, up, g):
        part = part_of(g)
        dst = (lo if up else hi).at[phase, :, part]
        r = (recv_lo if up else recv_hi).at[phase, g]
        return remote(relay.at[phase, :, part], dst, relay_out.at[phase, g], r,
                      group if up else -group)

    def detour(share, phase, g):
        left = chunks - 1 - g
        shift = 1 - phase
        return ((left + 1) * share + shift) // layers - (left * share + shift) // layers == 1

    def detour_up(phase, g):
        return detour(layers - 1 - layer, phase, g)

    def detour_dn(phase, g):
        return detour(layer, phase, g)

    def send(phase, g):
        for up, near, end, bent in (
            (True, has_hi, is_last, detour_up), (False, has_lo, is_first, detour_dn),
        ):
            if relays:
                by_relay = near & end & bent(phase, g)

                @pl.when(by_relay)
                def _(up=up):
                    main(phase, up, g, True).start()

                @pl.when(near & jnp.logical_not(by_relay))
                def _(up=up):
                    main(phase, up, g, False).start()
            else:
                @pl.when(near)
                def _(up=up):
                    main(phase, up, g, False).start()

            @pl.when(near)
            def _(up=up):
                tails(phase, up, g).start()

    def sent(phase, g):
        for up, near in ((True, has_hi), (False, has_lo)):
            @pl.when(near)
            def _(up=up):
                main(phase, up, g, False).wait_send()
                tails(phase, up, g).wait_send()

        if relays:
            for up, end, bent in ((True, is_first, detour_up), (False, is_last, detour_dn)):
                @pl.when(end & bent(phase, g))
                def _(up=up):
                    forward(phase, up, g).wait_send()

    def pass_on(phase, g):
        if relays:
            for up, end, bent in ((True, is_first, detour_up), (False, is_last, detour_dn)):
                @pl.when(end & bent(phase, g))
                def _(up=up):
                    main(phase, up, g, True).wait_recv()
                    forward(phase, up, g).start()

    def arrived(phase, g):
        for up, near in ((True, has_lo), (False, has_hi)):
            @pl.when(near)
            def _(up=up):
                main(phase, up, g, False).wait_recv()
                tails(phase, up, g).wait_recv()

    @pl.when(has_hi)
    def _():
        for c in flows(True):
            c.start()

    @pl.when(has_lo)
    def _():
        for c in flows(False):
            c.start()

    def begin(g, carry):
        @pl.when(g < chunks - 1)
        def _():
            reorder(g + 1)

        send(0, g)
        return carry

    lax.fori_loop(0, chunks, begin, 0)

    spans = [(q * LANES, min(LANES, nlon - q * LANES)) for q in range(width // LANES)]

    def tiles_of(x):
        lane = lax.broadcasted_iota(jnp.int32, (x.shape[0], LANES), 1)
        tiles = [x[:, q * LANES : (q + 1) * LANES] for q in range(width // LANES)]
        return tiles[:-1] + [jnp.where(lane < rest, tiles[-1], 0.0)]

    def fold(phase, g):
        part = part_of(g)
        own = first if phase else start
        x = jnp.concatenate([own[rows - 1 - k, part, :] for k in range(HALO)], axis=0)
        tiles = mirrored(tiles_of(x), nlon)
        for (at, n), t in zip(spans[:-1], tiles[:-1]):
            for k in range(HALO):
                hi[phase, k, part, at : at + n] = t[SUB * k : SUB * k + SUB]
        pack_hi[phase, g] = packed(tiles[-1][:SUB], tiles[-1][SUB:], rest)

    @pl.when(jnp.logical_not(has_lo))
    def _():
        v_lo[...] = jnp.zeros_like(v_lo)
        lev_lo[...] = jnp.zeros_like(lev_lo)
        lo[...] = jnp.zeros_like(lo)
        pack_lo[...] = jnp.zeros_like(pack_lo)

    @pl.when(jnp.logical_not(has_hi))
    def _():
        lev = jnp.broadcast_to(lev_ref[rows - 1 : rows, :].astype(jnp.float32), (SUB - levels, nlon))
        x = jnp.concatenate([flow[1, rows - 1], lev], axis=0)
        x = jnp.concatenate([x, jnp.zeros((SUB, width - nlon), jnp.float32)], axis=1)
        for (at, n), t in zip(spans, mirrored(tiles_of(x), nlon)):
            v_hi[:, at : at + n] = -t[:levels, :n]
            lev_hi[:, at : at + n] = (t[levels : levels + 1, :n] + 0.5).astype(jnp.int32)

        def fold_start(g, carry):
            fold(0, g)
            return carry

        lax.fori_loop(0, chunks, fold_start, 0)

    @pl.when(has_lo)
    def _():
        for c in flows(True):
            c.wait_recv()

    @pl.when(has_hi)
    def _():
        for c in flows(False):
            c.wait_recv()

    def shift(x, by):
        return pltpu.roll(x, (-by) % width, 1)

    wets[0] = wet_of(lev_lo[...])
    wets[rows + 1] = wet_of(lev_hi[...])

    def spread(x):
        return wrapped(jnp.concatenate([x] * (SUB // levels), axis=0), nlon)

    def v_row(j):
        if j < 0:
            return spread(v_lo[...])
        if j >= rows:
            return spread(v_hi[...])
        return spread(flow[1, j])

    def north_face(j):
        return face_terms(0.5 * (v_row(j) + v_row(j + 1)), wets[j + 1] * wets[j + 2])

    below = north_face(-1)
    for k in range(rows):
        wet = wets[k + 1]
        u = spread(flow[0, k])
        ea, eb, ed, ee = face_terms(0.5 * (u + shift(u, 1)), wet * shift(wet, 1))
        above = north_face(k)
        coef[k, 0] = wet * shift(ea, -1)
        coef[k, 1] = wet * (shift(eb, -1) - ea)
        coef[k, 2] = wet * (shift(ee, -1) - ed)
        coef[k, 3] = wet * -ee
        coef[k, 4] = wet * below[0]
        coef[k, 5] = wet * (below[1] - above[0])
        coef[k, 6] = wet * (below[3] - above[2])
        coef[k, 7] = wet * -above[3]
        coef[k, 8] = wet * (1.0 - eb + shift(ed, -1) - above[1] + below[2])
        below = above

    outer = [
        (k, 4 + i, k + d)
        for k in range(rows)
        for i, d in enumerate((-2, -1, 1, 2))
        if not 0 <= k + d < rows
    ]
    for n, (k, i, _) in enumerate(outer):
        edge[n] = 0.5 * coef[k, i]

    def section(get, k):
        f = get(k)
        total = coef[k, 8] * f
        total += coef[k, 0] * shift(f, -2)
        total += coef[k, 1] * shift(f, -1)
        total += coef[k, 2] * shift(f, 1)
        total += coef[k, 3] * shift(f, 2)
        for i, d in enumerate((-2, -1, 1, 2)):
            other = get(k + d)
            if other is not None:
                total += coef[k, 4 + i] * other
        return total

    def step(g, carry):
        pass_on(0, g)
        arrived(0, g)
        part = part_of(g)
        for low, mains, packs in ((0, lo, pack_lo), (HALO, hi, pack_hi)):
            for k, t in enumerate(unpacked(packs[0, g], rest)):
                halo[low + k] = joined(mains[0, k, part, :], t, rest)

        def field(j):
            if j < 0:
                return halo[j + HALO]
            if j >= rows:
                return halo[j - rows + HALO]
            return start[j, part, :]

        for k in range(rows):
            first[k, part, :] = section(field, k)
        put_packs(1, g, lambda k: first[k, part, whole:])

        def own(j):
            return first[j, part, :] if 0 <= j < rows else None

        for k in range(rows):
            partial[k, part, :] = 0.5 * (start[k, part, :] * wets[k + 1] + section(own, k))

        send(1, g)

        @pl.when(jnp.logical_not(has_hi))
        def _():
            fold(1, g)

        return carry

    lax.fori_loop(0, chunks, step, 0)

    def last(g, carry):
        pass_on(1, g)
        sent(0, g)
        arrived(1, g)
        part = part_of(g)
        others = {}
        for low, mains, packs in ((-HALO, lo, pack_lo), (rows, hi, pack_hi)):
            for k, t in enumerate(unpacked(packs[1, g], rest)):
                others[low + k] = jnp.concatenate([mains[1, k, part, :], t], axis=1)
        for k in range(rows):
            value = partial[k, part, :]
            for n, (at, _, j) in enumerate(outer):
                if at == k:
                    value += edge[n] * others[j]
            out_ref[part, k, :] = value[:, :nlon]
        return carry

    lax.fori_loop(0, chunks, last, 0)

    @pl.when(has_hi)
    def _():
        for c in flows(True):
            c.wait_send()

    @pl.when(has_lo)
    def _():
        for c in flows(False):
            c.wait_send()

    def finish(g, carry):
        sent(1, g)
        return carry

    lax.fori_loop(0, chunks, finish, 0)


def shards(group, tracers, currents, column_levels):
    count, levels, rows, nlon = tracers.shape
    planes = count * levels
    width = -(-(nlon + 2 * WRAP) // LANES) * LANES
    whole = nlon - nlon % LANES
    raw = tracers.reshape(planes, rows, nlon)
    chunks = planes // SUB
    hbm = pl.BlockSpec(memory_space=pltpu.HBM)
    vmem = pl.BlockSpec(memory_space=pltpu.VMEM)
    dma = pltpu.SemaphoreType.DMA

    def f32(*shape):
        return pltpu.VMEM(shape, jnp.float32)

    def i32(*shape):
        return pltpu.VMEM(shape, jnp.int32)

    pack = f32(2, chunks, SUB // 2, LANES)
    args = [pltpu.with_memory_space_constraint(x, pltpu.HBM) for x in (raw, currents, column_levels)]
    out = pl.pallas_call(
        functools.partial(kernel, nlon, levels, group),
        out_shape=jax.ShapeDtypeStruct((planes, rows, nlon), jnp.float32),
        in_specs=[hbm] * 3,
        out_specs=vmem,
        scratch_shapes=[
            f32(planes, rows, nlon),
            f32(*currents.shape),
            i32(*column_levels.shape),
            f32(rows, planes, width),
            f32(rows, planes, width),
            f32(rows, planes, width),
            f32(2, HALO, planes, whole),
            f32(2, HALO, planes, whole),
            f32(2, HALO, planes, whole),
            pack, pack, pack, pack,
            f32(2, rows, levels, nlon),
            f32(levels, nlon),
            f32(levels, nlon),
            i32(1, nlon), i32(1, nlon), i32(1, nlon), i32(1, nlon),
            f32(rows, 9, SUB, width),
            f32(6, SUB, width),
            f32(rows + 2, SUB, width),
            f32(2 * HALO, SUB, width),
            dma((chunks,)), dma((2,)),
        ] + [dma((2, chunks))] * 10 + [dma((4,)), dma((4,))],
        compiler_params=pltpu.CompilerParams(
            collective_id=0, has_side_effects=True, vmem_limit_bytes=44 * 1024 * 1024
        ),
    )(*args)
    return out.reshape(tracers.shape)


def layer_size(mesh):
    devices = mesh.devices.reshape(-1, mesh.shape["lat"])[0]
    spots = [getattr(d, "coords", None) for d in devices]
    if any(s is None or len(s) < 3 for s in spots):
        return 4
    return sum(s[2] == spots[0][2] for s in spots)


def solution(mesh):
    in_specs = (
        P("member", None, "lat", None),
        P("member", None, "lat", None),
        P(("member", "lat"), None),
    )
    out_specs = P("member", None, "lat", None)
    return jax.shard_map(
        functools.partial(shards, layer_size(mesh)),
        mesh=mesh, in_specs=in_specs, out_specs=out_specs, check_vma=False,
    )
```

```python
import functools

import jax
import jax.numpy as jnp
from jax import lax
from jax.experimental import pallas as pl
from jax.experimental.pallas import tpu as pltpu
from jax.sharding import PartitionSpec as P

LANES = 128
SUB = 8
WRAP = 4
HALO = 2
LEAD = 6
MESH = pl.DeviceIdType.MESH


def wrapped(x, nlon):
    rest = nlon % LANES
    whole = nlon - rest
    tail = jnp.concatenate([x[:, whole:], x[:, : LANES - rest]], axis=1)
    lane = lax.broadcasted_iota(jnp.int32, tail.shape, 1)
    tail = jnp.where(lane >= LANES - WRAP, pltpu.roll(tail, LANES - rest, 1), tail)
    return jnp.concatenate([x[:, :whole], tail], axis=1)


def joined(main, tail, rest):
    lane = lax.broadcasted_iota(jnp.int32, tail.shape, 1)
    west = pltpu.roll(tail, LANES - rest, 1)
    tail = jnp.where(lane < rest, tail, pltpu.roll(main[:, :LANES], rest, 1))
    tail = jnp.where(lane >= LANES - WRAP, west, tail)
    return jnp.concatenate([main, tail], axis=1)


def packed(a, b, rest):
    lane = lax.broadcasted_iota(jnp.int32, a.shape, 1)
    both = jnp.where(lane < rest, a, pltpu.roll(b, rest, 1))
    other = pltpu.roll(pltpu.roll(both, SUB // 2, 0), LANES // 2, 1)
    return jnp.where(lane < LANES // 2, both, other)[: SUB // 2]


def unpacked(half, rest):
    x = jnp.concatenate([half, half], axis=0)
    row = lax.broadcasted_iota(jnp.int32, x.shape, 0)
    x = jnp.where(row < SUB // 2, x, pltpu.roll(x, LANES // 2, 1))
    return x, pltpu.roll(x, LANES - rest, 1)


def face_terms(c, opened):
    c = c * opened * (1.0 / 12.0)
    m = jnp.abs(c)
    return -c - m, 7.0 * c + 3.0 * m, 7.0 * c - 3.0 * m, m - c


def mirrored(tiles, nlon):
    count = len(tiles)
    rest = nlon % LANES
    lane = lax.broadcasted_iota(jnp.int32, tiles[0].shape, 1)
    source = jnp.where(lane < rest, rest - 1 - lane, LANES + rest - 1 - lane)
    turned = [jnp.take_along_axis(t, source, axis=1, mode="promise_in_bounds") for t in tiles]
    return [
        jnp.where(lane < rest, turned[(count - 1 - q) % count], turned[(count - 2 - q) % count])
        for q in range(count)
    ]


def kernel(
    nlon, levels, group, raw_hbm, flow_hbm, lev_hbm, out_ref,
    raw, raw_flow, lev_ref, start, first, partial, lo, hi, relay, pack_up, pack_dn, pack_lo, pack_hi,
    flow, v_lo, v_hi, lev_up, lev_dn, lev_lo, lev_hi, coef, edge, wets, halo,
    load, aux_load, send_up, send_dn, recv_lo, recv_hi, relay_in, relay_out,
    psend_up, psend_dn, precv_lo, precv_hi, fsend, frecv,
):
    lat = lax.axis_size("lat")
    me = lax.axis_index("lat")
    rows, planes, width = start.shape
    rest = nlon % LANES
    whole = nlon - rest
    chunks = planes // SUB
    layers = lat // group
    layer = me // group
    place = me % group
    relays = layers > 1 and group > 2 and lat % group == 0
    has_lo = me > 0
    has_hi = me < lat - 1
    is_first = place == 0
    is_last = place == group - 1
    barrier = pltpu.get_barrier_semaphore()

    pairs = [(has_lo, -1), (has_hi, 1)]
    if relays:
        pairs += [
            (is_first, group - 1),
            (is_last, 1 - group),
            ((is_first | is_last) & (layer < layers - 1), group),
            ((is_first | is_last) & (layer > 0), -group),
        ]

    def part_of(g):
        return pl.ds(pl.multiple_of(g * SUB, SUB), SUB)

    def loading(g):
        part = part_of(g)
        return pltpu.make_async_copy(raw_hbm.at[part], raw.at[part], load.at[g])

    lev_load = pltpu.make_async_copy(lev_hbm, lev_ref, aux_load.at[0])
    flow_load = pltpu.make_async_copy(flow_hbm, raw_flow, aux_load.at[1])
    lev_load.start()
    loading(0).start()
    flow_load.start()

    for near, by in pairs:
        @pl.when(near)
        def _(by=by):
            pl.semaphore_signal(barrier, inc=1, device_id={"lat": me + by}, device_id_type=MESH)

    def load_rest(g, carry):
        loading(g).start()
        return carry

    lax.fori_loop(1, chunks, load_rest, 0)

    ranks = lax.rem(lax.broadcasted_iota(jnp.int32, (SUB, nlon), 0), levels)

    def wet_of(row):
        lev = jnp.broadcast_to(row, (SUB, nlon))
        return wrapped(jnp.where(ranks < lev, 1.0, 0.0), nlon)

    lev_load.wait()
    for k in range(rows):
        wets[k + 1] = wet_of(lev_ref[k : k + 1, :])
    lev_up[...] = lev_ref[rows - 1 : rows, :]
    lev_dn[...] = lev_ref[0:1, :]

    def put_packs(phase, g, tail):
        pack_up[phase, g] = packed(tail(rows - 2), tail(rows - 1), rest)
        pack_dn[phase, g] = packed(tail(0), tail(1), rest)

    def reorder(g):
        part = part_of(g)
        loading(g).wait()
        tails = []
        for k in range(rows):
            x = wrapped(raw[part, k, :], nlon) * wets[k + 1]
            start[k, part, :] = x
            tails.append(x[:, whole:])
        put_packs(0, g, lambda k: tails[k])

    reorder(0)
    flow_load.wait()
    for k in range(rows):
        for which in range(2):
            flow[which, k] = raw_flow[which, :, k, :]

    pl.semaphore_wait(barrier, sum(jnp.where(near, 1, 0) for near, _ in pairs))

    def remote(src, dst, s, r, by):
        return pltpu.make_async_remote_copy(
            src_ref=src, dst_ref=dst, send_sem=s, recv_sem=r,
            device_id={"lat": me + by}, device_id_type=MESH,
        )

    def flows(up):
        n = 0 if up else 2
        if up:
            pieces = [(flow.at[1, rows - 1], v_lo), (lev_up, lev_lo)]
        else:
            pieces = [(flow.at[1, 0], v_hi), (lev_dn, lev_hi)]
        by = 1 if up else -1
        return [
            remote(src, dst, fsend.at[n + i], frecv.at[n + i], by)
            for i, (src, dst) in enumerate(pieces)
        ]

    def main(phase, up, g, via):
        part = part_of(g)
        own = first if phase else start
        src = own.at[pl.ds(rows - HALO if up else 0, HALO), part, pl.ds(0, whole)]
        s = (send_up if up else send_dn).at[phase, g]
        if via:
            by = 1 - group if up else group - 1
            return remote(src, relay.at[phase, :, part], s, relay_in.at[phase, g], by)
        dst = (lo if up else hi).at[phase, :, part]
        r = (recv_lo if up else recv_hi).at[phase, g]
        return remote(src, dst, s, r, 1 if up else -1)

    def tails(phase, up, g):
        if up:
            return remote(pack_up.at[phase, g], pack_lo.at[phase, g],
                          psend_up.at[phase, g], precv_lo.at[phase, g], 1)
        return remote(pack_dn.at[phase, g], pack_hi.at[phase, g],
                      psend_dn.at[phase, g], precv_hi.at[phase, g], -1)

    def forward(phase, up, g):
        part = part_of(g)
        dst = (lo if up else hi).at[phase, :, part]
        r = (recv_lo if up else recv_hi).at[phase, g]
        return remote(relay.at[phase, :, part], dst, relay_out.at[phase, g], r,
                      group if up else -group)

    def detour(share, phase, g):
        left = chunks - 1 - g
        shift = 1 - phase
        return ((left + 1) * share + shift) // layers - (left * share + shift) // layers == 1

    def detour_up(phase, g):
        return detour(layers - 1 - layer, phase, g)

    def detour_dn(phase, g):
        return detour(layer, phase, g)

    def send(phase, g):
        for up, near, end, bent in (
            (True, has_hi, is_last, detour_up), (False, has_lo, is_first, detour_dn),
        ):
            if relays:
                by_relay = near & end & bent(phase, g)

                @pl.when(by_relay)
                def _(up=up):
                    main(phase, up, g, True).start()

                @pl.when(near & jnp.logical_not(by_relay))
                def _(up=up):
                    main(phase, up, g, False).start()
            else:
                @pl.when(near)
                def _(up=up):
                    main(phase, up, g, False).start()

            @pl.when(near)
            def _(up=up):
                tails(phase, up, g).start()

    def sent(phase, g):
        for up, near in ((True, has_hi), (False, has_lo)):
            @pl.when(near)
            def _(up=up):
                main(phase, up, g, False).wait_send()
                tails(phase, up, g).wait_send()

        if relays:
            for up, end, bent in ((True, is_first, detour_up), (False, is_last, detour_dn)):
                @pl.when(end & bent(phase, g))
                def _(up=up):
                    forward(phase, up, g).wait_send()

    def pass_on(phase, g):
        if relays:
            for up, end, bent in ((True, is_first, detour_up), (False, is_last, detour_dn)):
                @pl.when(end & bent(phase, g))
                def _(up=up):
                    main(phase, up, g, True).wait_recv()
                    forward(phase, up, g).start()

    lead = min(LEAD, chunks)

    def pass_first(phase):
        def one(g, carry):
            pass_on(phase, g)
            return carry

        lax.fori_loop(0, lead, one, 0)

    def pass_next(phase, g):
        @pl.when(g + lead < chunks)
        def _():
            pass_on(phase, g + lead)

    def arrived(phase, g):
        for up, near in ((True, has_lo), (False, has_hi)):
            @pl.when(near)
            def _(up=up):
                main(phase, up, g, False).wait_recv()
                tails(phase, up, g).wait_recv()

    @pl.when(has_hi)
    def _():
        for c in flows(True):
            c.start()

    @pl.when(has_lo)
    def _():
        for c in flows(False):
            c.start()

    def begin(g, carry):
        @pl.when(g < chunks - 1)
        def _():
            reorder(g + 1)

        send(0, g)
        return carry

    lax.fori_loop(0, chunks, begin, 0)

    spans = [(q * LANES, min(LANES, nlon - q * LANES)) for q in range(width // LANES)]

    def tiles_of(x):
        return [x[:, q * LANES : (q + 1) * LANES] for q in range(width // LANES)]

    def fold(phase, g):
        part = part_of(g)
        own = first if phase else start
        ends = []
        for k in range(HALO):
            tiles = mirrored(tiles_of(own[rows - 1 - k, part, :]), nlon)
            for (at, n), t in zip(spans[:-1], tiles[:-1]):
                hi[phase, k, part, at : at + n] = t
            ends.append(tiles[-1])
        pack_hi[phase, g] = packed(*ends, rest)

    @pl.when(jnp.logical_not(has_lo))
    def _():
        v_lo[...] = jnp.zeros_like(v_lo)
        lev_lo[...] = jnp.zeros_like(lev_lo)
        lo[...] = jnp.zeros_like(lo)
        pack_lo[...] = jnp.zeros_like(pack_lo)

    @pl.when(jnp.logical_not(has_hi))
    def _():
        lev = jnp.broadcast_to(lev_ref[rows - 1 : rows, :].astype(jnp.float32), (SUB - levels, nlon))
        x = jnp.concatenate([flow[1, rows - 1], lev], axis=0)
        x = jnp.concatenate([x, jnp.zeros((SUB, width - nlon), jnp.float32)], axis=1)
        for (at, n), t in zip(spans, mirrored(tiles_of(x), nlon)):
            v_hi[:, at : at + n] = -t[:levels, :n]
            lev_hi[:, at : at + n] = (t[levels : levels + 1, :n] + 0.5).astype(jnp.int32)

        def fold_start(g, carry):
            fold(0, g)
            return carry

        lax.fori_loop(0, chunks, fold_start, 0)

    @pl.when(has_lo)
    def _():
        for c in flows(True):
            c.wait_recv()

    @pl.when(has_hi)
    def _():
        for c in flows(False):
            c.wait_recv()

    def shift(x, by):
        return pltpu.roll(x, (-by) % width, 1)

    wets[0] = wet_of(lev_lo[...])
    wets[rows + 1] = wet_of(lev_hi[...])

    def spread(x):
        return wrapped(jnp.concatenate([x] * (SUB // levels), axis=0), nlon)

    def v_row(j):
        if j < 0:
            return spread(v_lo[...])
        if j >= rows:
            return spread(v_hi[...])
        return spread(flow[1, j])

    def north_face(j):
        return face_terms(0.5 * (v_row(j) + v_row(j + 1)), wets[j + 1] * wets[j + 2])

    below = north_face(-1)
    for k in range(rows):
        wet = wets[k + 1]
        u = spread(flow[0, k])
        ea, eb, ed, ee = face_terms(0.5 * (u + shift(u, 1)), wet * shift(wet, 1))
        above = north_face(k)
        coef[k, 0] = wet * shift(ea, -1)
        coef[k, 1] = wet * (shift(eb, -1) - ea)
        coef[k, 2] = wet * (shift(ee, -1) - ed)
        coef[k, 3] = wet * -ee
        coef[k, 4] = wet * below[0]
        coef[k, 5] = wet * (below[1] - above[0])
        coef[k, 6] = wet * (below[3] - above[2])
        coef[k, 7] = wet * -above[3]
        coef[k, 8] = wet * (1.0 - eb + shift(ed, -1) - above[1] + below[2])
        below = above

    outer = [
        (k, 4 + i, k + d)
        for k in range(rows)
        for i, d in enumerate((-2, -1, 1, 2))
        if not 0 <= k + d < rows
    ]
    for n, (k, i, _) in enumerate(outer):
        edge[n] = 0.5 * coef[k, i]

    def section(get, k):
        f = get(k)
        total = coef[k, 8] * f
        total += coef[k, 0] * shift(f, -2)
        total += coef[k, 1] * shift(f, -1)
        total += coef[k, 2] * shift(f, 1)
        total += coef[k, 3] * shift(f, 2)
        for i, d in enumerate((-2, -1, 1, 2)):
            other = get(k + d)
            if other is not None:
                total += coef[k, 4 + i] * other
        return total

    def step(g, carry):
        pass_next(0, g)
        arrived(0, g)
        part = part_of(g)
        for low, mains, packs in ((0, lo, pack_lo), (HALO, hi, pack_hi)):
            for k, t in enumerate(unpacked(packs[0, g], rest)):
                halo[low + k] = joined(mains[0, k, part, :], t, rest)

        def field(j):
            if j < 0:
                return halo[j + HALO]
            if j >= rows:
                return halo[j - rows + HALO]
            return start[j, part, :]

        for k in range(rows):
            first[k, part, :] = section(field, k)
        put_packs(1, g, lambda k: first[k, part, whole:])

        def own(j):
            return first[j, part, :] if 0 <= j < rows else None

        for k in range(rows):
            partial[k, part, :] = 0.5 * (start[k, part, :] * wets[k + 1] + section(own, k))

        send(1, g)

        @pl.when(jnp.logical_not(has_hi))
        def _():
            fold(1, g)

        return carry

    pass_first(0)
    lax.fori_loop(0, chunks, step, 0)

    def last(g, carry):
        pass_next(1, g)
        sent(0, g)
        arrived(1, g)
        part = part_of(g)
        others = {}
        for low, mains, packs in ((-HALO, lo, pack_lo), (rows, hi, pack_hi)):
            for k, t in enumerate(unpacked(packs[1, g], rest)):
                others[low + k] = jnp.concatenate([mains[1, k, part, :], t], axis=1)
        for k in range(rows):
            value = partial[k, part, :]
            for n, (at, _, j) in enumerate(outer):
                if at == k:
                    value += edge[n] * others[j]
            out_ref[part, k, :] = value[:, :nlon]
        return carry

    pass_first(1)
    lax.fori_loop(0, chunks, last, 0)

    @pl.when(has_hi)
    def _():
        for c in flows(True):
            c.wait_send()

    @pl.when(has_lo)
    def _():
        for c in flows(False):
            c.wait_send()

    def finish(g, carry):
        sent(1, g)
        return carry

    lax.fori_loop(0, chunks, finish, 0)


def shards(group, tracers, currents, column_levels):
    count, levels, rows, nlon = tracers.shape
    planes = count * levels
    width = -(-(nlon + 2 * WRAP) // LANES) * LANES
    whole = nlon - nlon % LANES
    raw = tracers.reshape(planes, rows, nlon)
    chunks = planes // SUB
    hbm = pl.BlockSpec(memory_space=pltpu.HBM)
    vmem = pl.BlockSpec(memory_space=pltpu.VMEM)
    dma = pltpu.SemaphoreType.DMA

    def f32(*shape):
        return pltpu.VMEM(shape, jnp.float32)

    def i32(*shape):
        return pltpu.VMEM(shape, jnp.int32)

    pack = f32(2, chunks, SUB // 2, LANES)
    args = [pltpu.with_memory_space_constraint(x, pltpu.HBM) for x in (raw, currents, column_levels)]
    out = pl.pallas_call(
        functools.partial(kernel, nlon, levels, group),
        out_shape=jax.ShapeDtypeStruct((planes, rows, nlon), jnp.float32),
        in_specs=[hbm] * 3,
        out_specs=vmem,
        scratch_shapes=[
            f32(planes, rows, nlon),
            f32(*currents.shape),
            i32(*column_levels.shape),
            f32(rows, planes, width),
            f32(rows, planes, width),
            f32(rows, planes, width),
            f32(2, HALO, planes, whole),
            f32(2, HALO, planes, whole),
            f32(2, HALO, planes, whole),
            pack, pack, pack, pack,
            f32(2, rows, levels, nlon),
            f32(levels, nlon),
            f32(levels, nlon),
            i32(1, nlon), i32(1, nlon), i32(1, nlon), i32(1, nlon),
            f32(rows, 9, SUB, width),
            f32(6, SUB, width),
            f32(rows + 2, SUB, width),
            f32(2 * HALO, SUB, width),
            dma((chunks,)), dma((2,)),
        ] + [dma((2, chunks))] * 10 + [dma((4,)), dma((4,))],
        compiler_params=pltpu.CompilerParams(
            collective_id=0, has_side_effects=True, vmem_limit_bytes=44 * 1024 * 1024
        ),
    )(*args)
    return out.reshape(tracers.shape)


def layer_size(mesh):
    devices = mesh.devices.reshape(-1, mesh.shape["lat"])[0]
    spots = [getattr(d, "coords", None) for d in devices]
    if any(s is None or len(s) < 3 for s in spots):
        return 4
    return sum(s[2] == spots[0][2] for s in spots)


def solution(mesh):
    in_specs = (
        P("member", None, "lat", None),
        P("member", None, "lat", None),
        P(("member", "lat"), None),
    )
    out_specs = P("member", None, "lat", None)
    return jax.shard_map(
        functools.partial(shards, layer_size(mesh)),
        mesh=mesh, in_specs=in_specs, out_specs=out_specs, check_vma=False,
    )
```

```python
import functools

import jax
import jax.numpy as jnp
from jax import lax
from jax.experimental import pallas as pl
from jax.experimental.pallas import tpu as pltpu
from jax.sharding import PartitionSpec as P

LANES = 128
SUB = 8
WRAP = 4
HALO = 2
LEAD = 2
WIDEST = 3
PACK_CUT = 3
MESH = pl.DeviceIdType.MESH


def wrapped(x, nlon):
    rest = nlon % LANES
    whole = nlon - rest
    tail = jnp.concatenate([x[:, whole:], x[:, : LANES - rest]], axis=1)
    lane = lax.broadcasted_iota(jnp.int32, tail.shape, 1)
    tail = jnp.where(lane >= LANES - WRAP, pltpu.roll(tail, LANES - rest, 1), tail)
    return jnp.concatenate([x[:, :whole], tail], axis=1)


def joined(main, tail, rest):
    lane = lax.broadcasted_iota(jnp.int32, tail.shape, 1)
    west = pltpu.roll(tail, LANES - rest, 1)
    tail = jnp.where(lane < rest, tail, pltpu.roll(main[:, :LANES], rest, 1))
    tail = jnp.where(lane >= LANES - WRAP, west, tail)
    return jnp.concatenate([main, tail], axis=1)


def packed(a, b, rest):
    lane = lax.broadcasted_iota(jnp.int32, a.shape, 1)
    both = jnp.where(lane < rest, a, pltpu.roll(b, rest, 1))
    other = pltpu.roll(pltpu.roll(both, SUB // 2, 0), LANES // 2, 1)
    return jnp.where(lane < LANES // 2, both, other)[: SUB // 2]


def unpacked(half, rest):
    x = jnp.concatenate([half, half], axis=0)
    row = lax.broadcasted_iota(jnp.int32, x.shape, 0)
    x = jnp.where(row < SUB // 2, x, pltpu.roll(x, LANES // 2, 1))
    return x, pltpu.roll(x, LANES - rest, 1)


def face_terms(c, opened):
    c = c * opened * (1.0 / 12.0)
    m = jnp.abs(c)
    return -c - m, 7.0 * c + 3.0 * m, 7.0 * c - 3.0 * m, m - c


def mirrored(tiles, nlon):
    count = len(tiles)
    rest = nlon % LANES
    lane = lax.broadcasted_iota(jnp.int32, tiles[0].shape, 1)
    source = jnp.where(lane < rest, rest - 1 - lane, LANES + rest - 1 - lane)
    turned = [jnp.take_along_axis(t, source, axis=1, mode="promise_in_bounds") for t in tiles]
    return [
        jnp.where(lane < rest, turned[(count - 1 - q) % count], turned[(count - 2 - q) % count])
        for q in range(count)
    ]


def growing(n):
    sizes, step = [], 1
    while sum(sizes) < n:
        sizes.append(min(step, n - sum(sizes)))
        step = min(2 * step, WIDEST)
    return sizes


def spans_of(sizes):
    return [(sum(sizes[:i]), n) for i, n in enumerate(sizes)]


def detours(sizes, layers):
    names = [(phase, i) for phase in range(2) for i in range(len(sizes[phase]))][:-1]
    result = []
    for share in range(layers):
        goal = sum(sizes[0] + sizes[1]) * share / layers
        best = None
        for bits in range(2 ** len(names)):
            chosen = [name for n, name in enumerate(names) if bits >> n & 1]
            load = [sum(sizes[p][i] for p, i in chosen if p == phase) for phase in range(2)]
            late = sum(i for _, i in chosen)
            cost = (abs(sum(load) - goal), abs(load[0] - goal / 2), late)
            if best is None or cost < best[0]:
                best = (cost, chosen)
        result.append(best[1])
    return result


def kernel(
    nlon, levels, group, sizes, raw_hbm, flow_hbm, lev_hbm, out_ref,
    raw, raw_flow, lev_ref, start, first, partial, lo, hi, relay, pack_up, pack_dn, pack_lo, pack_hi,
    flow, v_lo, v_hi, lev_up, lev_dn, lev_lo, lev_hi, coef, edge, wets, halo,
    load, aux_load, send_up, send_dn, recv_lo, recv_hi, relay_in, relay_out,
    psend_up, psend_dn, precv_lo, precv_hi, fsend, frecv,
):
    lat = lax.axis_size("lat")
    me = lax.axis_index("lat")
    rows, planes, width = start.shape
    rest = nlon % LANES
    whole = nlon - rest
    chunks = planes // SUB
    groups = [spans_of(x) for x in sizes]
    cut = min(PACK_CUT, chunks - 1)
    packs = [[(0, cut), (cut, chunks - cut)], [(0, chunks - cut), (chunks - cut, cut)]]
    layers = lat // group
    layer = me // group
    place = me % group
    relays = layers > 1 and group > 2 and lat % group == 0
    has_lo = me > 0
    has_hi = me < lat - 1
    is_first = place == 0
    is_last = place == group - 1
    barrier = pltpu.get_barrier_semaphore()

    pairs = [(has_lo, -1), (has_hi, 1)]
    if relays:
        pairs += [
            (is_first, group - 1),
            (is_last, 1 - group),
            ((is_first | is_last) & (layer < layers - 1), group),
            ((is_first | is_last) & (layer > 0), -group),
        ]

    def part_of(g):
        return pl.ds(pl.multiple_of(g * SUB, SUB), SUB)

    def loading(i):
        at, n = groups[0][i]
        part = pl.ds(at * SUB, n * SUB)
        return pltpu.make_async_copy(raw_hbm.at[part], raw.at[part], load.at[i])

    lev_load = pltpu.make_async_copy(lev_hbm, lev_ref, aux_load.at[0])
    flow_load = pltpu.make_async_copy(flow_hbm, raw_flow, aux_load.at[1])
    lev_load.start()
    loading(0).start()
    flow_load.start()

    for near, by in pairs:
        @pl.when(near)
        def _(by=by):
            pl.semaphore_signal(barrier, inc=1, device_id={"lat": me + by}, device_id_type=MESH)

    for i in range(1, len(groups[0])):
        loading(i).start()

    ranks = lax.rem(lax.broadcasted_iota(jnp.int32, (SUB, nlon), 0), levels)

    def wet_of(row):
        lev = jnp.broadcast_to(row, (SUB, nlon))
        return wrapped(jnp.where(ranks < lev, 1.0, 0.0), nlon)

    lev_load.wait()
    for k in range(rows):
        wets[k + 1] = wet_of(lev_ref[k : k + 1, :])
    lev_up[...] = lev_ref[rows - 1 : rows, :]
    lev_dn[...] = lev_ref[0:1, :]

    def put_packs(phase, g, tail):
        pack_up[phase, g] = packed(tail(rows - 2), tail(rows - 1), rest)
        pack_dn[phase, g] = packed(tail(0), tail(1), rest)

    def reorder(g):
        part = part_of(g)
        ends = []
        for k in range(rows):
            x = wrapped(raw[part, k, :], nlon) * wets[k + 1]
            start[k, part, :] = x
            ends.append(x[:, whole:])
        put_packs(0, g, lambda k: ends[k])

    loading(0).wait()
    reorder(0)
    flow_load.wait()
    for k in range(rows):
        for which in range(2):
            flow[which, k] = raw_flow[which, :, k, :]

    pl.semaphore_wait(barrier, sum(jnp.where(near, 1, 0) for near, _ in pairs))

    def remote(src, dst, s, r, by):
        return pltpu.make_async_remote_copy(
            src_ref=src, dst_ref=dst, send_sem=s, recv_sem=r,
            device_id={"lat": me + by}, device_id_type=MESH,
        )

    def flows(up):
        n = 0 if up else 2
        if up:
            pieces = [(flow.at[1, rows - 1], v_lo), (lev_up, lev_lo)]
        else:
            pieces = [(flow.at[1, 0], v_hi), (lev_dn, lev_hi)]
        by = 1 if up else -1
        return [
            remote(src, dst, fsend.at[n + i], frecv.at[n + i], by)
            for i, (src, dst) in enumerate(pieces)
        ]

    def main(phase, up, i, via=False):
        at, n = (0, chunks) if i is None else groups[phase][i]
        part = pl.ds(at * SUB, n * SUB)
        own = first if phase else start
        src = own.at[pl.ds(rows - HALO if up else 0, HALO), part, pl.ds(0, whole)]
        s = (send_up if up else send_dn).at[phase]
        i = i or 0
        if via:
            by = 1 - group if up else group - 1
            return remote(src, relay.at[phase, :, part], s, relay_in.at[phase, i], by)
        dst = (lo if up else hi).at[phase, :, part]
        r = (recv_lo if up else recv_hi).at[phase, i]
        return remote(src, dst, s, r, 1 if up else -1)

    def ends_copy(phase, up, i):
        at, n = (0, chunks) if i is None else packs[phase][i]
        part = pl.ds(at, n)
        i = i or 0
        if up:
            return remote(pack_up.at[phase, part], pack_lo.at[phase, part],
                          psend_up.at[phase], precv_lo.at[phase, i], 1)
        return remote(pack_dn.at[phase, part], pack_hi.at[phase, part],
                      psend_dn.at[phase], precv_hi.at[phase, i], -1)

    def forward(phase, up, i):
        at, n = groups[phase][i]
        part = pl.ds(at * SUB, n * SUB)
        dst = (lo if up else hi).at[phase, :, part]
        r = (recv_lo if up else recv_hi).at[phase, i]
        return remote(relay.at[phase, :, part], dst, relay_out.at[phase, i], r,
                      group if up else -group)

    table = detours(sizes, layers) if relays else []

    def bent(phase, i, share):
        result = False
        for value, chosen in enumerate(table):
            if (phase, i) in chosen:
                result = result | (share == value)
        return result

    bent_up = {(p, i): bent(p, i, layers - 1 - layer) for p in range(2) for i in range(len(sizes[p]))}
    bent_dn = {(p, i): bent(p, i, layer) for p in range(2) for i in range(len(sizes[p]))}
    ways = ((True, has_hi, is_last, bent_up), (False, has_lo, is_first, bent_dn))
    duties = ((True, is_first, bent_up), (False, is_last, bent_dn))

    def send(phase, i):
        for up, near, end, flags in ways:
            flag = flags[phase, i]
            if flag is False:
                @pl.when(near)
                def _(up=up):
                    main(phase, up, i).start()
            else:
                by_relay = near & end & flag

                @pl.when(by_relay)
                def _(up=up):
                    main(phase, up, i, True).start()

                @pl.when(near & jnp.logical_not(by_relay))
                def _(up=up):
                    main(phase, up, i).start()

    def send_ends(phase, i):
        for up, near, _, _ in ways:
            @pl.when(near)
            def _(up=up):
                ends_copy(phase, up, i).start()

    def pass_on(phase, i):
        for up, end, flags in duties:
            flag = flags[phase, i]
            if flag is not False:
                @pl.when(end & flag)
                def _(up=up):
                    main(phase, up, i, True).wait_recv()
                    forward(phase, up, i).start()

    def passed(phase, i):
        for up, end, flags in duties:
            flag = flags[phase, i]
            if flag is not False:
                @pl.when(end & flag)
                def _(up=up):
                    forward(phase, up, i).wait_send()

    def arrived(copy, phase, i):
        for up, near in ((True, has_lo), (False, has_hi)):
            @pl.when(near)
            def _(up=up):
                copy(phase, up, i).wait_recv()

    def receive(phase, g):
        for i, (at, _) in enumerate(groups[phase]):
            @pl.when(g == at)
            def _(i=i):
                if i == 0:
                    for j in range(min(LEAD, len(groups[phase]))):
                        pass_on(phase, j)
                if i + LEAD < len(groups[phase]):
                    pass_on(phase, i + LEAD)
                arrived(main, phase, i)

        for i, (at, _) in enumerate(packs[phase]):
            @pl.when(g == at)
            def _(i=i):
                arrived(ends_copy, phase, i)

    def dispatch(phase, g):
        for i, (at, n) in enumerate(groups[phase]):
            @pl.when(g == at + n - 1)
            def _(i=i):
                send(phase, i)

        for i, (at, n) in enumerate(packs[phase]):
            @pl.when(g == at + n - 1)
            def _(i=i):
                send_ends(phase, i)

    send(0, 0)

    @pl.when(has_hi)
    def _():
        for c in flows(True):
            c.start()

    @pl.when(has_lo)
    def _():
        for c in flows(False):
            c.start()

    def begin(g, carry):
        for i, (at, _) in enumerate(groups[0]):
            if i:
                @pl.when(g == at)
                def _(i=i):
                    loading(i).wait()

        reorder(g)

        @pl.when(g > 1)
        def _():
            dispatch(0, g - 1)

        return carry

    lax.fori_loop(1, chunks, begin, 0)
    dispatch(0, chunks - 1)

    spans = [(q * LANES, min(LANES, nlon - q * LANES)) for q in range(width // LANES)]

    def tiles_of(x):
        return [x[:, q * LANES : (q + 1) * LANES] for q in range(width // LANES)]

    def fold(phase, g):
        part = part_of(g)
        own = first if phase else start
        ends = []
        for k in range(HALO):
            tiles = mirrored(tiles_of(own[rows - 1 - k, part, :]), nlon)
            for (at, n), t in zip(spans[:-1], tiles[:-1]):
                hi[phase, k, part, at : at + n] = t
            ends.append(tiles[-1])
        pack_hi[phase, g] = packed(*ends, rest)

    @pl.when(jnp.logical_not(has_lo))
    def _():
        v_lo[...] = jnp.zeros_like(v_lo)
        lev_lo[...] = jnp.zeros_like(lev_lo)
        lo[...] = jnp.zeros_like(lo)
        pack_lo[...] = jnp.zeros_like(pack_lo)

    @pl.when(jnp.logical_not(has_hi))
    def _():
        lev = jnp.broadcast_to(lev_ref[rows - 1 : rows, :].astype(jnp.float32), (SUB - levels, nlon))
        x = jnp.concatenate([flow[1, rows - 1], lev], axis=0)
        x = jnp.concatenate([x, jnp.zeros((SUB, width - nlon), jnp.float32)], axis=1)
        for (at, n), t in zip(spans, mirrored(tiles_of(x), nlon)):
            v_hi[:, at : at + n] = -t[:levels, :n]
            lev_hi[:, at : at + n] = (t[levels : levels + 1, :n] + 0.5).astype(jnp.int32)

        def fold_start(g, carry):
            fold(0, g)
            return carry

        lax.fori_loop(0, chunks, fold_start, 0)

    @pl.when(has_lo)
    def _():
        for c in flows(True):
            c.wait_recv()

    @pl.when(has_hi)
    def _():
        for c in flows(False):
            c.wait_recv()

    def shift(x, by):
        return pltpu.roll(x, (-by) % width, 1)

    wets[0] = wet_of(lev_lo[...])
    wets[rows + 1] = wet_of(lev_hi[...])

    def spread(x):
        return wrapped(jnp.concatenate([x] * (SUB // levels), axis=0), nlon)

    def v_row(j):
        if j < 0:
            return spread(v_lo[...])
        if j >= rows:
            return spread(v_hi[...])
        return spread(flow[1, j])

    def north_face(j):
        return face_terms(0.5 * (v_row(j) + v_row(j + 1)), wets[j + 1] * wets[j + 2])

    below = north_face(-1)
    for k in range(rows):
        wet = wets[k + 1]
        u = spread(flow[0, k])
        ea, eb, ed, ee = face_terms(0.5 * (u + shift(u, 1)), wet * shift(wet, 1))
        above = north_face(k)
        coef[k, 0] = wet * shift(ea, -1)
        coef[k, 1] = wet * (shift(eb, -1) - ea)
        coef[k, 2] = wet * (shift(ee, -1) - ed)
        coef[k, 3] = wet * -ee
        coef[k, 4] = wet * below[0]
        coef[k, 5] = wet * (below[1] - above[0])
        coef[k, 6] = wet * (below[3] - above[2])
        coef[k, 7] = wet * -above[3]
        coef[k, 8] = wet * (1.0 - eb + shift(ed, -1) - above[1] + below[2])
        below = above

    outer = [
        (k, 4 + i, k + d)
        for k in range(rows)
        for i, d in enumerate((-2, -1, 1, 2))
        if not 0 <= k + d < rows
    ]
    for n, (k, i, _) in enumerate(outer):
        edge[n] = 0.5 * coef[k, i]

    def section(get, k):
        f = get(k)
        total = coef[k, 8] * f
        total += coef[k, 0] * shift(f, -2)
        total += coef[k, 1] * shift(f, -1)
        total += coef[k, 2] * shift(f, 1)
        total += coef[k, 3] * shift(f, 2)
        for i, d in enumerate((-2, -1, 1, 2)):
            other = get(k + d)
            if other is not None:
                total += coef[k, 4 + i] * other
        return total

    def step(g, carry):
        receive(0, g)
        part = part_of(g)
        for low, mains, ends in ((0, lo, pack_lo), (HALO, hi, pack_hi)):
            for k, t in enumerate(unpacked(ends[0, g], rest)):
                halo[low + k] = joined(mains[0, k, part, :], t, rest)

        def field(j):
            if j < 0:
                return halo[j + HALO]
            if j >= rows:
                return halo[j - rows + HALO]
            return start[j, part, :]

        for k in range(rows):
            first[k, part, :] = section(field, k)
        put_packs(1, g, lambda k: first[k, part, whole:])

        def own(j):
            return first[j, part, :] if 0 <= j < rows else None

        for k in range(rows):
            partial[k, part, :] = 0.5 * (start[k, part, :] * wets[k + 1] + section(own, k))

        dispatch(1, g)

        @pl.when(jnp.logical_not(has_hi))
        def _():
            fold(1, g)

        return carry

    lax.fori_loop(0, chunks, step, 0)

    def last(g, carry):
        receive(1, g)
        part = part_of(g)
        others = {}
        for low, mains, ends in ((-HALO, lo, pack_lo), (rows, hi, pack_hi)):
            for k, t in enumerate(unpacked(ends[1, g], rest)):
                others[low + k] = jnp.concatenate([mains[1, k, part, :], t], axis=1)
        for k in range(rows):
            value = partial[k, part, :]
            for n, (at, _, j) in enumerate(outer):
                if at == k:
                    value += edge[n] * others[j]
            out_ref[part, k, :] = value[:, :nlon]
        return carry

    lax.fori_loop(0, chunks, last, 0)

    for up, near, _, _ in ways:
        @pl.when(near)
        def _(up=up):
            for c in flows(up):
                c.wait_send()
            for phase in range(2):
                main(phase, up, None).wait_send()
                ends_copy(phase, up, None).wait_send()

    for phase in range(2):
        for i in range(len(groups[phase])):
            passed(phase, i)


def shards(group, tracers, currents, column_levels):
    count, levels, rows, nlon = tracers.shape
    planes = count * levels
    width = -(-(nlon + 2 * WRAP) // LANES) * LANES
    whole = nlon - nlon % LANES
    raw = tracers.reshape(planes, rows, nlon)
    chunks = planes // SUB
    sizes = [growing(chunks), growing(chunks)[::-1]]
    count = len(sizes[0])
    hbm = pl.BlockSpec(memory_space=pltpu.HBM)
    vmem = pl.BlockSpec(memory_space=pltpu.VMEM)
    dma = pltpu.SemaphoreType.DMA

    def f32(*shape):
        return pltpu.VMEM(shape, jnp.float32)

    def i32(*shape):
        return pltpu.VMEM(shape, jnp.int32)

    pack = f32(2, chunks, SUB // 2, LANES)
    args = [pltpu.with_memory_space_constraint(x, pltpu.HBM) for x in (raw, currents, column_levels)]
    out = pl.pallas_call(
        functools.partial(kernel, nlon, levels, group, sizes),
        out_shape=jax.ShapeDtypeStruct((planes, rows, nlon), jnp.float32),
        in_specs=[hbm] * 3,
        out_specs=vmem,
        scratch_shapes=[
            f32(planes, rows, nlon),
            f32(*currents.shape),
            i32(*column_levels.shape),
            f32(rows, planes, width),
            f32(rows, planes, width),
            f32(rows, planes, width),
            f32(2, HALO, planes, whole),
            f32(2, HALO, planes, whole),
            f32(2, HALO, planes, whole),
            pack, pack, pack, pack,
            f32(2, rows, levels, nlon),
            f32(levels, nlon),
            f32(levels, nlon),
            i32(1, nlon), i32(1, nlon), i32(1, nlon), i32(1, nlon),
            f32(rows, 9, SUB, width),
            f32(6, SUB, width),
            f32(rows + 2, SUB, width),
            f32(2 * HALO, SUB, width),
            dma((count,)), dma((2,)), dma((2,)), dma((2,)),
            dma((2, count)), dma((2, count)), dma((2, count)), dma((2, count)),
            dma((2,)), dma((2,)), dma((2, 2)), dma((2, 2)), dma((4,)), dma((4,)),
        ],
        compiler_params=pltpu.CompilerParams(
            collective_id=0, has_side_effects=True, vmem_limit_bytes=44 * 1024 * 1024
        ),
    )(*args)
    return out.reshape(tracers.shape)


def layer_size(mesh):
    devices = mesh.devices.reshape(-1, mesh.shape["lat"])[0]
    spots = [getattr(d, "coords", None) for d in devices]
    if any(s is None or len(s) < 3 for s in spots):
        return 4
    return sum(s[2] == spots[0][2] for s in spots)


def solution(mesh):
    in_specs = (
        P("member", None, "lat", None),
        P("member", None, "lat", None),
        P(("member", "lat"), None),
    )
    out_specs = P("member", None, "lat", None)
    return jax.shard_map(
        functools.partial(shards, layer_size(mesh)),
        mesh=mesh, in_specs=in_specs, out_specs=out_specs, check_vma=False,
    )
```

```python
import functools

import jax
import jax.numpy as jnp
from jax import lax
from jax.experimental import pallas as pl
from jax.experimental.pallas import tpu as pltpu
from jax.sharding import PartitionSpec as P

LANES = 128
SUB = 8
WRAP = 4
HALO = 2
LEAD = 3
WIDEST = 2
PACK_CUT = 3
AHEAD = 2
MESH = pl.DeviceIdType.MESH


def wrapped(x, nlon):
    rest = nlon % LANES
    whole = nlon - rest
    tail = jnp.concatenate([x[:, whole:], x[:, : LANES - rest]], axis=1)
    lane = lax.broadcasted_iota(jnp.int32, tail.shape, 1)
    tail = jnp.where(lane >= LANES - WRAP, pltpu.roll(tail, LANES - rest, 1), tail)
    return jnp.concatenate([x[:, :whole], tail], axis=1)


def joined(main, tail, rest):
    lane = lax.broadcasted_iota(jnp.int32, tail.shape, 1)
    west = pltpu.roll(tail, LANES - rest, 1)
    tail = jnp.where(lane < rest, tail, pltpu.roll(main[:, :LANES], rest, 1))
    tail = jnp.where(lane >= LANES - WRAP, west, tail)
    return jnp.concatenate([main, tail], axis=1)


def packed(a, b, rest):
    lane = lax.broadcasted_iota(jnp.int32, a.shape, 1)
    both = jnp.where(lane < rest, a, pltpu.roll(b, rest, 1))
    other = pltpu.roll(pltpu.roll(both, SUB // 2, 0), LANES // 2, 1)
    return jnp.where(lane < LANES // 2, both, other)[: SUB // 2]


def unpacked(half, rest):
    x = jnp.concatenate([half, half], axis=0)
    row = lax.broadcasted_iota(jnp.int32, x.shape, 0)
    x = jnp.where(row < SUB // 2, x, pltpu.roll(x, LANES // 2, 1))
    return x, pltpu.roll(x, LANES - rest, 1)


def face_terms(c, opened):
    c = c * opened * (1.0 / 12.0)
    m = jnp.abs(c)
    return -c - m, 7.0 * c + 3.0 * m, 7.0 * c - 3.0 * m, m - c


def mirrored(tiles, nlon):
    count = len(tiles)
    rest = nlon % LANES
    lane = lax.broadcasted_iota(jnp.int32, tiles[0].shape, 1)
    source = jnp.where(lane < rest, rest - 1 - lane, LANES + rest - 1 - lane)
    turned = [jnp.take_along_axis(t, source, axis=1, mode="promise_in_bounds") for t in tiles]
    return [
        jnp.where(lane < rest, turned[(count - 1 - q) % count], turned[(count - 2 - q) % count])
        for q in range(count)
    ]


def growing(n, step):
    sizes = []
    while sum(sizes) < n:
        sizes.append(min(step, n - sum(sizes)))
        step = min(step + 1, WIDEST)
    return sizes


def spans_of(sizes):
    return [(sum(sizes[:i]), n) for i, n in enumerate(sizes)]


def detours(sizes, layers):
    names = [(phase, i) for phase in range(2) for i in range(len(sizes[phase]))][1:-2]
    result = []
    for share in range(layers):
        goal = sum(sizes[0] + sizes[1]) * share / layers
        best = None
        for bits in range(2 ** len(names)):
            chosen = [name for n, name in enumerate(names) if bits >> n & 1]
            load = [sum(sizes[p][i] for p, i in chosen if p == phase) for phase in range(2)]
            late = sum(i for _, i in chosen)
            cost = (abs(sum(load) - goal), abs(load[0] - goal / 2), late)
            if best is None or cost < best[0]:
                best = (cost, chosen)
        result.append(best[1])
    return result


def kernel(
    nlon, levels, group, sizes, raw_hbm, flow_hbm, lev_hbm, out_ref,
    raw, raw_flow, lev_ref, raw_lo, raw_hi, start, first, partial, lo, hi, relay, pack_up, pack_dn, pack_lo, pack_hi,
    flow, v_lo, v_hi, lev_lo, lev_hi, coef, edge, wets, halo,
    load, aux_load, send_up, send_dn, recv_lo, recv_hi, relay_in, relay_out,
    psend_up, psend_dn, precv_lo, precv_hi, fsend, frecv, send_raw,
):
    lat = lax.axis_size("lat")
    me = lax.axis_index("lat")
    rows, planes, width = start.shape
    rest = nlon % LANES
    whole = nlon - rest
    chunks = planes // SUB
    groups = [spans_of(x) for x in sizes]
    cut = min(PACK_CUT, chunks - 1)
    packs = [[(0, cut), (cut, chunks - cut)], [(0, chunks - cut), (chunks - cut, cut)]]
    layers = lat // group
    layer = me // group
    place = me % group
    relays = layers > 1 and group > 2 and lat % group == 0
    has_lo = me > 0
    has_hi = me < lat - 1
    is_first = place == 0
    is_last = place == group - 1
    barrier = pltpu.get_barrier_semaphore()

    pairs = [(has_lo, -1), (has_hi, 1)]
    if relays:
        pairs += [
            (is_first, group - 1),
            (is_last, 1 - group),
            ((is_first | is_last) & (layer < layers - 1), group),
            ((is_first | is_last) & (layer > 0), -group),
        ]

    def part_of(g):
        return pl.ds(pl.multiple_of(g * SUB, SUB), SUB)

    def loading(i):
        at, n = groups[0][i]
        part = pl.ds(at * SUB, n * SUB)
        return pltpu.make_async_copy(raw_hbm.at[part], raw.at[part], load.at[i])

    lev_load = pltpu.make_async_copy(lev_hbm, lev_ref, aux_load.at[0])
    flow_load = pltpu.make_async_copy(flow_hbm, raw_flow, aux_load.at[1])
    for near, by in pairs:
        @pl.when(near)
        def _(by=by):
            pl.semaphore_signal(barrier, inc=1, device_id={"lat": me + by}, device_id_type=MESH)

    lev_load.start()
    loading(0).start()
    flow_load.start()

    for i in range(1, len(groups[0])):
        loading(i).start()

    def remote(src, dst, s, r, by):
        return pltpu.make_async_remote_copy(
            src_ref=src, dst_ref=dst, send_sem=s, recv_sem=r,
            device_id={"lat": me + by}, device_id_type=MESH,
        )

    def flows(up):
        n = 0 if up else 2
        k = rows - 1 if up else 0
        levs = lev_hbm.at[pl.ds(rows - HALO if up else 0, HALO)]
        pieces = [(flow_hbm.at[1, :, k], v_lo if up else v_hi), (levs, lev_lo if up else lev_hi)]
        by = 1 if up else -1
        return [
            remote(src, dst, fsend.at[n + i], frecv.at[n + i], by)
            for i, (src, dst) in enumerate(pieces)
        ]

    def unmasked(up):
        n = groups[0][0][1] * SUB
        src = raw_hbm.at[pl.ds(0, n), pl.ds(rows - HALO if up else 0, HALO), pl.ds(0, whole)]
        s, r = (send_raw.at[0], recv_lo.at[0, 0]) if up else (send_raw.at[1], recv_hi.at[0, 0])
        return remote(src, raw_lo if up else raw_hi, s, r, 1 if up else -1)

    def main(phase, up, i, via=False):
        skip = 0 if phase else groups[0][0][1]
        at, n = (skip, chunks - skip) if i is None else groups[phase][i]
        part = pl.ds(at * SUB, n * SUB)
        own = first if phase else start
        src = own.at[pl.ds(rows - HALO if up else 0, HALO), part, pl.ds(0, whole)]
        s = (send_up if up else send_dn).at[phase]
        i = i or 0
        if via:
            by = 1 - group if up else group - 1
            return remote(src, relay.at[phase, :, part], s, relay_in.at[phase, i], by)
        dst = (lo if up else hi).at[phase, :, part]
        r = (recv_lo if up else recv_hi).at[phase, i]
        return remote(src, dst, s, r, 1 if up else -1)

    def ends_copy(phase, up, i):
        at, n = (0, chunks) if i is None else packs[phase][i]
        part = pl.ds(at, n)
        i = i or 0
        if up:
            return remote(pack_up.at[phase, part], pack_lo.at[phase, part],
                          psend_up.at[phase], precv_lo.at[phase, i], 1)
        return remote(pack_dn.at[phase, part], pack_hi.at[phase, part],
                      psend_dn.at[phase], precv_hi.at[phase, i], -1)

    def forward(phase, up, i):
        at, n = groups[phase][i]
        part = pl.ds(at * SUB, n * SUB)
        dst = (lo if up else hi).at[phase, :, part]
        r = (recv_lo if up else recv_hi).at[phase, i]
        return remote(relay.at[phase, :, part], dst, relay_out.at[phase], r,
                      group if up else -group)

    table = detours(sizes, layers) if relays else []

    def bent(phase, i, share):
        result = False
        for value, chosen in enumerate(table):
            if (phase, i) in chosen:
                result = result | (share == value)
        return result

    bent_up = {(p, i): bent(p, i, layers - 1 - layer) for p in range(2) for i in range(len(sizes[p]))}
    bent_dn = {(p, i): bent(p, i, layer) for p in range(2) for i in range(len(sizes[p]))}
    ways = ((True, has_hi, is_last, bent_up), (False, has_lo, is_first, bent_dn))
    duties = ((True, is_first, bent_up), (False, is_last, bent_dn))

    def send(phase, i):
        for up, near, end, flags in ways:
            flag = flags[phase, i]
            if flag is False:
                @pl.when(near)
                def _(up=up):
                    main(phase, up, i).start()
            else:
                by_relay = near & end & flag

                @pl.when(by_relay)
                def _(up=up):
                    main(phase, up, i, True).start()

                @pl.when(near & jnp.logical_not(by_relay))
                def _(up=up):
                    main(phase, up, i).start()

    def send_ends(phase, i):
        for up, near, _, _ in ways:
            @pl.when(near)
            def _(up=up):
                ends_copy(phase, up, i).start()

    def pass_on(phase, i):
        if i:
            passed(phase, i - 1)
        for up, end, flags in duties:
            flag = flags[phase, i]
            if flag is not False:
                @pl.when(end & flag)
                def _(up=up):
                    main(phase, up, i, True).wait_recv()
                    forward(phase, up, i).start()

    def passed(phase, i):
        for up, end, flags in duties:
            flag = flags[phase, i]
            if flag is not False:
                @pl.when(end & flag)
                def _(up=up):
                    forward(phase, up, i).wait_send()

    def arrived(copy, phase, i):
        for up, near in ((True, has_lo), (False, has_hi)):
            @pl.when(near)
            def _(up=up):
                copy(phase, up, i).wait_recv()

    def receive(phase, g):
        for i, (at, _) in enumerate(groups[phase]):
            @pl.when(g == at)
            def _(i=i):
                if i == 0:
                    for j in range(min(LEAD, len(groups[phase]))):
                        pass_on(phase, j)
                if i + LEAD < len(groups[phase]):
                    pass_on(phase, i + LEAD)
                arrived(main if phase or i else lambda phase, up, i: unmasked(up), phase, i)

        for i, (at, _) in enumerate(packs[phase]):
            @pl.when(g == at)
            def _(i=i):
                arrived(ends_copy, phase, i)

    def dispatch(phase, g):
        for i, (at, n) in enumerate(groups[phase]):
            if phase or i:
                @pl.when(g == at + n - 1)
                def _(i=i):
                    send(phase, i)

        for i, (at, n) in enumerate(packs[phase]):
            @pl.when(g == at + n - 1)
            def _(i=i):
                send_ends(phase, i)

    pl.semaphore_wait(barrier, sum(jnp.where(near, 1, 0) for near, _ in pairs))

    for up, near, _, _ in ways:
        @pl.when(near)
        def _(up=up):
            unmasked(up).start()
            for c in flows(up):
                c.start()

    ranks = lax.rem(lax.broadcasted_iota(jnp.int32, (SUB, nlon), 0), levels)

    def wet_of(row):
        lev = jnp.broadcast_to(row, (SUB, nlon))
        return wrapped(jnp.where(ranks < lev, 1.0, 0.0), nlon)

    lev_load.wait()
    for k in range(rows):
        wets[k + 1] = wet_of(lev_ref[k : k + 1, :])

    def put_packs(phase, g, tail):
        pack_up[phase, g] = packed(tail(rows - 2), tail(rows - 1), rest)
        pack_dn[phase, g] = packed(tail(0), tail(1), rest)

    def reorder(g):
        part = part_of(g)
        ends = []
        for k in range(rows):
            x = wrapped(raw[part, k, :], nlon) * wets[k + 1]
            start[k, part, :] = x
            ends.append(x[:, whole:])
        put_packs(0, g, lambda k: ends[k])

    loading(0).wait()
    reorder(0)
    flow_load.wait()
    for k in range(rows):
        for which in range(2):
            flow[which, k] = raw_flow[which, :, k, :]

    def begin(g, carry):
        for i, (at, _) in enumerate(groups[0]):
            if i:
                @pl.when(g == at)
                def _(i=i):
                    loading(i).wait()

        reorder(g)

        @pl.when(g > 1)
        def _():
            dispatch(0, g - 1)

        return carry

    lax.fori_loop(1, chunks, begin, 0)
    dispatch(0, chunks - 1)

    spans = [(q * LANES, min(LANES, nlon - q * LANES)) for q in range(width // LANES)]

    def tiles_of(x):
        return [x[:, q * LANES : (q + 1) * LANES] for q in range(width // LANES)]

    def fold(phase, g):
        part = part_of(g)
        own = first if phase else start
        ends = []
        for k in range(HALO):
            tiles = mirrored(tiles_of(own[rows - 1 - k, part, :]), nlon)
            for (at, n), t in zip(spans[:-1], tiles[:-1]):
                hi[phase, k, part, at : at + n] = t
            ends.append(tiles[-1])
        pack_hi[phase, g] = packed(*ends, rest)

    @pl.when(jnp.logical_not(has_lo))
    def _():
        v_lo[...] = jnp.zeros_like(v_lo)
        lev_lo[...] = jnp.zeros_like(lev_lo)
        lo[...] = jnp.zeros_like(lo)
        pack_lo[...] = jnp.zeros_like(pack_lo)

    @pl.when(jnp.logical_not(has_hi))
    def _():
        lev = jnp.broadcast_to(lev_ref[rows - 1 : rows, :].astype(jnp.float32), (SUB - levels, nlon))
        x = jnp.concatenate([flow[1, rows - 1], lev], axis=0)
        x = jnp.concatenate([x, jnp.zeros((SUB, width - nlon), jnp.float32)], axis=1)
        for (at, n), t in zip(spans, mirrored(tiles_of(x), nlon)):
            v_hi[:, at : at + n] = -t[:levels, :n]
            lev_hi[0:1, at : at + n] = (t[levels : levels + 1, :n] + 0.5).astype(jnp.int32)

        def fold_start(g, carry):
            fold(0, g)
            return carry

        lax.fori_loop(0, chunks, fold_start, 0)

    @pl.when(has_lo)
    def _():
        for c in flows(True):
            c.wait_recv()

    @pl.when(has_hi)
    def _():
        for c in flows(False):
            c.wait_recv()

    def shift(x, by):
        return pltpu.roll(x, (-by) % width, 1)

    wets[0] = wet_of(lev_lo[HALO - 1 : HALO, :])
    wets[rows + 1] = wet_of(lev_hi[0:1, :])

    def spread(x):
        return wrapped(jnp.concatenate([x] * (SUB // levels), axis=0), nlon)

    def v_row(j):
        if j < 0:
            return spread(v_lo[...])
        if j >= rows:
            return spread(v_hi[...])
        return spread(flow[1, j])

    def north_face(j):
        return face_terms(0.5 * (v_row(j) + v_row(j + 1)), wets[j + 1] * wets[j + 2])

    below = north_face(-1)
    for k in range(rows):
        wet = wets[k + 1]
        u = spread(flow[0, k])
        ea, eb, ed, ee = face_terms(0.5 * (u + shift(u, 1)), wet * shift(wet, 1))
        above = north_face(k)
        coef[k, 0] = wet * shift(ea, -1)
        coef[k, 1] = wet * (shift(eb, -1) - ea)
        coef[k, 2] = wet * (shift(ee, -1) - ed)
        coef[k, 3] = wet * -ee
        coef[k, 4] = wet * below[0]
        coef[k, 5] = wet * (below[1] - above[0])
        coef[k, 6] = wet * (below[3] - above[2])
        coef[k, 7] = wet * -above[3]
        coef[k, 8] = wet * (1.0 - eb + shift(ed, -1) - above[1] + below[2])
        below = above

    outer = [
        (k, 4 + i, k + d)
        for k in range(rows)
        for i, d in enumerate((-2, -1, 1, 2))
        if not 0 <= k + d < rows
    ]
    for n, (k, i, _) in enumerate(outer):
        edge[n] = 0.5 * coef[k, i]

    def section(get, k):
        f = get(k)
        total = coef[k, 8] * f
        total += coef[k, 0] * shift(f, -2)
        total += coef[k, 1] * shift(f, -1)
        total += coef[k, 2] * shift(f, 1)
        total += coef[k, 3] * shift(f, 2)
        for i, d in enumerate((-2, -1, 1, 2)):
            other = get(k + d)
            if other is not None:
                total += coef[k, 4 + i] * other
        return total

    def mask_first(g):
        part = part_of(g)
        for near, source, levs, mains in ((has_lo, raw_lo, lev_lo, lo), (has_hi, raw_hi, lev_hi, hi)):
            @pl.when(near)
            def _(source=source, levs=levs, mains=mains):
                for k in range(HALO):
                    wet = jnp.where(ranks < jnp.broadcast_to(levs[k : k + 1, :], (SUB, nlon)), 1.0, 0.0)
                    mains[0, k, part, :] = source[part, k, :] * wet[:, :whole]

    def step(g, carry):
        receive(0, g)

        @pl.when(g < groups[0][0][1])
        def _():
            mask_first(g)

        part = part_of(g)
        for low, mains, ends in ((0, lo, pack_lo), (HALO, hi, pack_hi)):
            for k, t in enumerate(unpacked(ends[0, g], rest)):
                halo[low + k] = joined(mains[0, k, part, :], t, rest)

        def field(j):
            if j < 0:
                return halo[j + HALO]
            if j >= rows:
                return halo[j - rows + HALO]
            return start[j, part, :]

        for k in range(rows):
            first[k, part, :] = section(field, k)
        put_packs(1, g, lambda k: first[k, part, whole:])

        def own(j):
            return first[j, part, :] if 0 <= j < rows else None

        for k in range(rows):
            partial[k, part, :] = 0.5 * (start[k, part, :] * wets[k + 1] + section(own, k))

        dispatch(1, g)

        @pl.when(jnp.logical_not(has_hi))
        def _():
            fold(1, g)

        return carry

    lax.fori_loop(0, chunks, step, 0)

    def last(g, carry):
        receive(1, g)
        part = part_of(g)
        others = {}
        for low, mains, ends in ((-HALO, lo, pack_lo), (rows, hi, pack_hi)):
            for k, t in enumerate(unpacked(ends[1, g], rest)):
                others[low + k] = jnp.concatenate([mains[1, k, part, :], t], axis=1)
        for k in range(rows):
            value = partial[k, part, :]
            for n, (at, _, j) in enumerate(outer):
                if at == k:
                    value += edge[n] * others[j]
            out_ref[part, k, :] = value[:, :nlon]
        return carry

    lax.fori_loop(0, chunks, last, 0)

    for up, near, _, _ in ways:
        @pl.when(near)
        def _(up=up):
            for c in [unmasked(up)] + flows(up):
                c.wait_send()
            for phase in range(2):
                main(phase, up, None).wait_send()
                ends_copy(phase, up, None).wait_send()

    for phase in range(2):
        passed(phase, len(groups[phase]) - 1)


def shards(group, tracers, currents, column_levels):
    count, levels, rows, nlon = tracers.shape
    planes = count * levels
    width = -(-(nlon + 2 * WRAP) // LANES) * LANES
    whole = nlon - nlon % LANES
    raw = tracers.reshape(planes, rows, nlon)
    chunks = planes // SUB
    sizes = [growing(chunks, AHEAD), growing(chunks, 1)[::-1]]
    count = max(map(len, sizes))
    hbm = pl.BlockSpec(memory_space=pltpu.HBM)
    vmem = pl.BlockSpec(memory_space=pltpu.VMEM)
    dma = pltpu.SemaphoreType.DMA

    def f32(*shape):
        return pltpu.VMEM(shape, jnp.float32)

    def i32(*shape):
        return pltpu.VMEM(shape, jnp.int32)

    pack = f32(2, chunks, SUB // 2, LANES)
    args = [pltpu.with_memory_space_constraint(x, pltpu.HBM) for x in (raw, currents, column_levels)]
    out = pl.pallas_call(
        functools.partial(kernel, nlon, levels, group, sizes),
        out_shape=jax.ShapeDtypeStruct((planes, rows, nlon), jnp.float32),
        in_specs=[hbm] * 3,
        out_specs=vmem,
        scratch_shapes=[
            f32(planes, rows, nlon),
            f32(*currents.shape),
            i32(*column_levels.shape),
            f32(sizes[0][0] * SUB, HALO, whole),
            f32(sizes[0][0] * SUB, HALO, whole),
            f32(rows, planes, width),
            f32(rows, planes, width),
            f32(rows, planes, width),
            f32(2, HALO, planes, whole),
            f32(2, HALO, planes, whole),
            f32(2, HALO, planes, whole),
            pack, pack, pack, pack,
            f32(2, rows, levels, nlon),
            f32(levels, nlon),
            f32(levels, nlon),
            i32(HALO, nlon), i32(HALO, nlon),
            f32(rows, 9, SUB, width),
            f32(6, SUB, width),
            f32(rows + 2, SUB, width),
            f32(2 * HALO, SUB, width),
            dma((len(sizes[0]),)), dma((2,)), dma((2,)), dma((2,)),
            dma((2, count)), dma((2, count)), dma((2, count)), dma((2,)),
            dma((2,)), dma((2,)), dma((2, 2)), dma((2, 2)), dma((4,)), dma((4,)), dma((2,)),
        ],
        compiler_params=pltpu.CompilerParams(
            collective_id=0, has_side_effects=True, vmem_limit_bytes=44 * 1024 * 1024
        ),
    )(*args)
    return out.reshape(tracers.shape)


def layer_size(mesh):
    devices = mesh.devices.reshape(-1, mesh.shape["lat"])[0]
    spots = [getattr(d, "coords", None) for d in devices]
    if any(s is None or len(s) < 3 for s in spots):
        return 4
    return sum(s[2] == spots[0][2] for s in spots)


def solution(mesh):
    in_specs = (
        P("member", None, "lat", None),
        P("member", None, "lat", None),
        P(("member", "lat"), None),
    )
    out_specs = P("member", None, "lat", None)
    return jax.shard_map(
        functools.partial(shards, layer_size(mesh)),
        mesh=mesh, in_specs=in_specs, out_specs=out_specs, check_vma=False,
    )
```

```python
import functools

import jax
import jax.numpy as jnp
from jax import lax
from jax.experimental import pallas as pl
from jax.experimental.pallas import tpu as pltpu
from jax.sharding import PartitionSpec as P

LANES = 128
SUB = 8
WRAP = 4
HALO = 2
LEAD = 2, 1
WIDEST = 4
PACK_CUT = 3
AHEAD = 2
KEEP = 2
DIRECT = 0.0
MESH = pl.DeviceIdType.MESH


def wrapped(x, nlon):
    rest = nlon % LANES
    whole = nlon - rest
    tail = jnp.concatenate([x[:, whole:], x[:, : LANES - rest]], axis=1)
    lane = lax.broadcasted_iota(jnp.int32, tail.shape, 1)
    tail = jnp.where(lane >= LANES - WRAP, pltpu.roll(tail, LANES - rest, 1), tail)
    return jnp.concatenate([x[:, :whole], tail], axis=1)


def joined(main, tail, rest):
    lane = lax.broadcasted_iota(jnp.int32, tail.shape, 1)
    west = pltpu.roll(tail, LANES - rest, 1)
    tail = jnp.where(lane < rest, tail, pltpu.roll(main[:, :LANES], rest, 1))
    tail = jnp.where(lane >= LANES - WRAP, west, tail)
    return jnp.concatenate([main, tail], axis=1)


def packed(a, b, rest):
    lane = lax.broadcasted_iota(jnp.int32, a.shape, 1)
    both = jnp.where(lane < rest, a, pltpu.roll(b, rest, 1))
    other = pltpu.roll(pltpu.roll(both, SUB // 2, 0), LANES // 2, 1)
    return jnp.where(lane < LANES // 2, both, other)[: SUB // 2]


def unpacked(half, rest):
    x = jnp.concatenate([half, half], axis=0)
    row = lax.broadcasted_iota(jnp.int32, x.shape, 0)
    x = jnp.where(row < SUB // 2, x, pltpu.roll(x, LANES // 2, 1))
    return x, pltpu.roll(x, LANES - rest, 1)


def face_terms(c, opened):
    c = c * opened * (1.0 / 12.0)
    m = jnp.abs(c)
    return -c - m, 7.0 * c + 3.0 * m, 7.0 * c - 3.0 * m, m - c


def mirrored(tiles, nlon):
    count = len(tiles)
    rest = nlon % LANES
    lane = lax.broadcasted_iota(jnp.int32, tiles[0].shape, 1)
    source = jnp.where(lane < rest, rest - 1 - lane, LANES + rest - 1 - lane)
    turned = [jnp.take_along_axis(t, source, axis=1, mode="promise_in_bounds") for t in tiles]
    return [
        jnp.where(lane < rest, turned[(count - 1 - q) % count], turned[(count - 2 - q) % count])
        for q in range(count)
    ]


def growing(n, step):
    sizes = []
    while sum(sizes) < n:
        sizes.append(min(step, n - sum(sizes)))
        step = min(step + 1, WIDEST)
    return sizes


def spans_of(sizes):
    return [(sum(sizes[:i]), n) for i, n in enumerate(sizes)]


def load_sizes(chunks):
    rest = chunks - AHEAD
    return [AHEAD, rest // 3, rest - rest // 3]


def pack_sizes(chunks):
    early = [PACK_CUT]
    while sum(early) < chunks:
        early.append(min(PACK_CUT + 1, chunks - sum(early)))
    return [early, early[::-1]]


def pieces_of(chunks):
    sizes = [AHEAD, 1] + growing(chunks - AHEAD - 3, WIDEST) + [1, 1]
    early = [(at, n, 0, HALO) for at, n in spans_of(sizes)]
    at, n, _, _ = early.pop()
    early += [(at, n, k, 1) for k in range(HALO)]
    late = [(at, n, 0, HALO) for at, n in spans_of(growing(chunks, 1)[::-1])]
    return [early, late]


def subsets(items):
    best = {0: []}
    for size, name in items:
        for total, chosen in list(best.items()):
            best.setdefault(total + size, chosen + [name])
    return best


def detours(groups, layers):
    size = {(p, i): n * k / HALO for p in range(2) for i, (_, n, _, k) in enumerate(groups[p])}
    names = list(size)[1:-KEEP]
    choices = [subsets([(size[n], n) for n in names if n[0] == phase]) for phase in range(2)]
    result = []
    for share in range(layers):
        goal = (sum(size.values()) + DIRECT) * share / layers
        _, one, two = min(
            ((abs(one + two - goal), abs(one - goal / 2)), one, two)
            for one in choices[0] for two in choices[1]
        )
        result.append(choices[0][one] + choices[1][two] if share else [])
    return result


def kernel(
    nlon, levels, group, groups, table, raw_hbm, flow_hbm, lev_hbm, out_ref,
    raw, raw_flow, lev_ref, raw_lo, raw_hi, start, first, partial, lo, hi, relay, pack_up, pack_dn, pack_lo, pack_hi,
    flow, v_lo, v_hi, lev_lo, lev_hi, coef, edge, wets, halo,
    load, aux_load, send_up, send_dn, recv_lo, recv_hi, relay_in, relay_out,
    psend_up, psend_dn, precv_lo, precv_hi, fsend, frecv, send_raw,
):
    lat = lax.axis_size("lat")
    me = lax.axis_index("lat")
    rows, planes, width = start.shape
    rest = nlon % LANES
    whole = nlon - rest
    chunks = planes // SUB
    loads = spans_of(load_sizes(chunks))
    offset = [0, len(groups[0])]
    packs = [spans_of(x) for x in pack_sizes(chunks)]
    first_pack = [0, len(packs[0])]
    layers = lat // group
    layer = me // group
    place = me % group
    relays = bool(table)
    has_lo = me > 0
    has_hi = me < lat - 1
    is_first = place == 0
    is_last = place == group - 1
    barrier = pltpu.get_barrier_semaphore()

    pairs = [(has_lo, -1), (has_hi, 1)]
    if relays:
        pairs += [
            (is_first, group - 1),
            (is_last, 1 - group),
            ((is_first | is_last) & (layer < layers - 1), group),
            ((is_first | is_last) & (layer > 0), -group),
        ]

    def part_of(g):
        return pl.ds(pl.multiple_of(g * SUB, SUB), SUB)

    def loading(i):
        at, n = loads[i]
        part = pl.ds(at * SUB, n * SUB)
        return pltpu.make_async_copy(raw_hbm.at[part], raw.at[part], load.at[i])

    lev_load = pltpu.make_async_copy(lev_hbm, lev_ref, aux_load.at[0])
    flow_load = pltpu.make_async_copy(flow_hbm, raw_flow, aux_load.at[1])
    for near, by in pairs:
        @pl.when(near)
        def _(by=by):
            pl.semaphore_signal(barrier, inc=1, device_id={"lat": me + by}, device_id_type=MESH)

    lev_load.start()
    loading(0).start()
    flow_load.start()

    for i in range(1, len(loads)):
        loading(i).start()

    def remote(src, dst, s, r, by):
        return pltpu.make_async_remote_copy(
            src_ref=src, dst_ref=dst, send_sem=s, recv_sem=r,
            device_id={"lat": me + by}, device_id_type=MESH,
        )

    def flows(up):
        n = 0 if up else 2
        k = rows - 1 if up else 0
        levs = lev_hbm.at[pl.ds(rows - HALO if up else 0, HALO)]
        pieces = [(flow_hbm.at[1, :, k], v_lo if up else v_hi), (levs, lev_lo if up else lev_hi)]
        by = 1 if up else -1
        return [
            remote(src, dst, fsend.at[n + i], frecv.at[n + i], by)
            for i, (src, dst) in enumerate(pieces)
        ]

    def unmasked(up):
        n = groups[0][0][1] * SUB
        src = raw_hbm.at[pl.ds(0, n), pl.ds(rows - HALO if up else 0, HALO), pl.ds(0, whole)]
        s, r = (send_raw.at[0], recv_lo.at[0]) if up else (send_raw.at[1], recv_hi.at[0])
        return remote(src, raw_lo if up else raw_hi, s, r, 1 if up else -1)

    def main(phase, up, i, via=False):
        skip = 0 if phase else groups[0][0][1]
        at, n, k, count = (skip, chunks - skip, 0, HALO) if i is None else groups[phase][i]
        part = pl.ds(at * SUB, n * SUB)
        own = first if phase else start
        src = own.at[pl.ds(k + (rows - HALO if up else 0), count), part, pl.ds(0, whole)]
        s = (send_up if up else send_dn).at[phase]
        r = offset[phase] + (i or 0)
        if via:
            by = 1 - group if up else group - 1
            return remote(src, relay.at[phase, pl.ds(k, count), part], s, relay_in.at[r], by)
        dst = (lo if up else hi).at[phase, pl.ds(k, count), part]
        return remote(src, dst, s, (recv_lo if up else recv_hi).at[r], 1 if up else -1)

    def ends_copy(phase, up, i):
        at, n = (0, chunks) if i is None else packs[phase][i]
        part = pl.ds(at, n)
        i = first_pack[phase] + (i or 0)
        if up:
            return remote(pack_up.at[phase, part], pack_lo.at[phase, part],
                          psend_up.at[phase], precv_lo.at[i], 1)
        return remote(pack_dn.at[phase, part], pack_hi.at[phase, part],
                      psend_dn.at[phase], precv_hi.at[i], -1)

    def forward(phase, up, i):
        at, n, k, count = groups[phase][i]
        part = pl.ds(at * SUB, n * SUB)
        piece = pl.ds(k, count)
        dst = (lo if up else hi).at[phase, piece, part]
        r = (recv_lo if up else recv_hi).at[offset[phase] + i]
        return remote(relay.at[phase, piece, part], dst, relay_out.at[phase], r,
                      group if up else -group)

    def bent(phase, i, share):
        result = False
        for value, chosen in enumerate(table):
            if (phase, i) in chosen:
                result = result | (share == value)
        return result

    names = [(p, i) for p in range(2) for i in range(len(groups[p]))]
    bent_up = {name: bent(*name, layers - 1 - layer) for name in names}
    bent_dn = {name: bent(*name, layer) for name in names}
    ways = ((True, has_hi, is_last, bent_up), (False, has_lo, is_first, bent_dn))
    duties = ((True, is_first, bent_up), (False, is_last, bent_dn))

    def send(phase, i):
        for up, near, end, flags in ways:
            flag = flags[phase, i]
            if flag is False:
                @pl.when(near)
                def _(up=up):
                    main(phase, up, i).start()
            else:
                by_relay = near & end & flag

                @pl.when(by_relay)
                def _(up=up):
                    main(phase, up, i, True).start()

                @pl.when(near & jnp.logical_not(by_relay))
                def _(up=up):
                    main(phase, up, i).start()

    def send_ends(phase, i):
        for up, near, _, _ in ways:
            @pl.when(near)
            def _(up=up):
                ends_copy(phase, up, i).start()

    def pass_on(phase, i):
        if i:
            passed(phase, i - 1)
        for up, end, flags in duties:
            flag = flags[phase, i]
            if flag is not False:
                @pl.when(end & flag)
                def _(up=up):
                    main(phase, up, i, True).wait_recv()
                    forward(phase, up, i).start()

    def passed(phase, i):
        for up, end, flags in duties:
            flag = flags[phase, i]
            if flag is not False:
                @pl.when(end & flag)
                def _(up=up):
                    forward(phase, up, i).wait_send()

    def arrived(copy, phase, i):
        for up, near in ((True, has_lo), (False, has_hi)):
            @pl.when(near)
            def _(up=up):
                copy(phase, up, i).wait_recv()

    def receive(phase, g):
        for i, (at, _, _, _) in enumerate(groups[phase]):
            @pl.when(g == at)
            def _(i=i):
                if i == 0:
                    for j in range(min(LEAD[phase], len(groups[phase]))):
                        pass_on(phase, j)
                if i + LEAD[phase] < len(groups[phase]):
                    pass_on(phase, i + LEAD[phase])
                arrived(main if phase or i else lambda phase, up, i: unmasked(up), phase, i)

        for i, (at, _) in enumerate(packs[phase]):
            @pl.when(g == at)
            def _(i=i):
                arrived(ends_copy, phase, i)

    def dispatch(phase, g):
        for i, (at, n, _, _) in enumerate(groups[phase]):
            if phase or i:
                @pl.when(g == at + n - 1)
                def _(i=i):
                    send(phase, i)

        for i, (at, n) in enumerate(packs[phase]):
            @pl.when(g == at + n - 1)
            def _(i=i):
                send_ends(phase, i)

    pl.semaphore_wait(barrier, sum(jnp.where(near, 1, 0) for near, _ in pairs))

    for up, near, _, _ in ways:
        @pl.when(near)
        def _(up=up):
            unmasked(up).start()
            for c in flows(up):
                c.start()

    ranks = lax.rem(lax.broadcasted_iota(jnp.int32, (SUB, nlon), 0), levels)

    def wet_of(row):
        lev = jnp.broadcast_to(row, (SUB, nlon))
        return wrapped(jnp.where(ranks < lev, 1.0, 0.0), nlon)

    lev_load.wait()
    for k in range(rows):
        wets[k + 1] = wet_of(lev_ref[k : k + 1, :])

    def put_packs(phase, g, tail):
        pack_up[phase, g] = packed(tail(rows - 2), tail(rows - 1), rest)
        pack_dn[phase, g] = packed(tail(0), tail(1), rest)

    def reorder(g):
        part = part_of(g)
        ends = []
        for k in range(rows):
            x = wrapped(raw[part, k, :], nlon) * wets[k + 1]
            start[k, part, :] = x
            ends.append(x[:, whole:])
        put_packs(0, g, lambda k: ends[k])

    loading(0).wait()
    reorder(0)
    flow_load.wait()
    for k in range(rows):
        for which in range(2):
            flow[which, k] = raw_flow[which, :, k, :]

    def begin(g, carry):
        for i, (at, _) in enumerate(loads):
            if i:
                @pl.when(g == at)
                def _(i=i):
                    loading(i).wait()

        reorder(g)

        @pl.when(g > 1)
        def _():
            dispatch(0, g - 1)

        return carry

    lax.fori_loop(1, chunks, begin, 0)
    dispatch(0, chunks - 1)

    spans = [(q * LANES, min(LANES, nlon - q * LANES)) for q in range(width // LANES)]

    def tiles_of(x):
        return [x[:, q * LANES : (q + 1) * LANES] for q in range(width // LANES)]

    def fold(phase, g):
        part = part_of(g)
        own = first if phase else start
        ends = []
        for k in range(HALO):
            tiles = mirrored(tiles_of(own[rows - 1 - k, part, :]), nlon)
            for (at, n), t in zip(spans[:-1], tiles[:-1]):
                hi[phase, k, part, at : at + n] = t
            ends.append(tiles[-1])
        pack_hi[phase, g] = packed(*ends, rest)

    @pl.when(jnp.logical_not(has_lo))
    def _():
        v_lo[...] = jnp.zeros_like(v_lo)
        lev_lo[...] = jnp.zeros_like(lev_lo)
        lo[...] = jnp.zeros_like(lo)
        pack_lo[...] = jnp.zeros_like(pack_lo)

    @pl.when(jnp.logical_not(has_hi))
    def _():
        lev = jnp.broadcast_to(lev_ref[rows - 1 : rows, :].astype(jnp.float32), (SUB - levels, nlon))
        x = jnp.concatenate([flow[1, rows - 1], lev], axis=0)
        x = jnp.concatenate([x, jnp.zeros((SUB, width - nlon), jnp.float32)], axis=1)
        for (at, n), t in zip(spans, mirrored(tiles_of(x), nlon)):
            v_hi[:, at : at + n] = -t[:levels, :n]
            lev_hi[0:1, at : at + n] = (t[levels : levels + 1, :n] + 0.5).astype(jnp.int32)

        def fold_start(g, carry):
            fold(0, g)
            return carry

        lax.fori_loop(0, chunks, fold_start, 0)

    @pl.when(has_lo)
    def _():
        for c in flows(True):
            c.wait_recv()

    @pl.when(has_hi)
    def _():
        for c in flows(False):
            c.wait_recv()

    def shift(x, by):
        return pltpu.roll(x, (-by) % width, 1)

    wets[0] = wet_of(lev_lo[HALO - 1 : HALO, :])
    wets[rows + 1] = wet_of(lev_hi[0:1, :])

    def spread(x):
        return wrapped(jnp.concatenate([x] * (SUB // levels), axis=0), nlon)

    def v_row(j):
        if j < 0:
            return spread(v_lo[...])
        if j >= rows:
            return spread(v_hi[...])
        return spread(flow[1, j])

    def north_face(j):
        return face_terms(0.5 * (v_row(j) + v_row(j + 1)), wets[j + 1] * wets[j + 2])

    below = north_face(-1)
    for k in range(rows):
        wet = wets[k + 1]
        u = spread(flow[0, k])
        ea, eb, ed, ee = face_terms(0.5 * (u + shift(u, 1)), wet * shift(wet, 1))
        above = north_face(k)
        coef[k, 0] = wet * shift(ea, -1)
        coef[k, 1] = wet * (shift(eb, -1) - ea)
        coef[k, 2] = wet * (shift(ee, -1) - ed)
        coef[k, 3] = wet * -ee
        coef[k, 4] = wet * below[0]
        coef[k, 5] = wet * (below[1] - above[0])
        coef[k, 6] = wet * (below[3] - above[2])
        coef[k, 7] = wet * -above[3]
        coef[k, 8] = wet * (1.0 - eb + shift(ed, -1) - above[1] + below[2])
        below = above

    outer = [
        (k, 4 + i, k + d)
        for k in range(rows)
        for i, d in enumerate((-2, -1, 1, 2))
        if not 0 <= k + d < rows
    ]
    for n, (k, i, _) in enumerate(outer):
        edge[n] = 0.5 * coef[k, i]

    def section(get, k):
        f = get(k)
        total = coef[k, 8] * f
        total += coef[k, 0] * shift(f, -2)
        total += coef[k, 1] * shift(f, -1)
        total += coef[k, 2] * shift(f, 1)
        total += coef[k, 3] * shift(f, 2)
        for i, d in enumerate((-2, -1, 1, 2)):
            other = get(k + d)
            if other is not None:
                total += coef[k, 4 + i] * other
        return total

    def mask_first(g):
        part = part_of(g)
        for near, source, levs, mains in ((has_lo, raw_lo, lev_lo, lo), (has_hi, raw_hi, lev_hi, hi)):
            @pl.when(near)
            def _(source=source, levs=levs, mains=mains):
                for k in range(HALO):
                    wet = jnp.where(ranks < jnp.broadcast_to(levs[k : k + 1, :], (SUB, nlon)), 1.0, 0.0)
                    mains[0, k, part, :] = source[part, k, :] * wet[:, :whole]

    def step(g, carry):
        receive(0, g)

        @pl.when(g < groups[0][0][1])
        def _():
            mask_first(g)

        part = part_of(g)
        for low, mains, ends in ((0, lo, pack_lo), (HALO, hi, pack_hi)):
            for k, t in enumerate(unpacked(ends[0, g], rest)):
                halo[low + k] = joined(mains[0, k, part, :], t, rest)

        def field(j):
            if j < 0:
                return halo[j + HALO]
            if j >= rows:
                return halo[j - rows + HALO]
            return start[j, part, :]

        for k in range(rows):
            first[k, part, :] = section(field, k)
        put_packs(1, g, lambda k: first[k, part, whole:])

        def own(j):
            return first[j, part, :] if 0 <= j < rows else None

        for k in range(rows):
            partial[k, part, :] = 0.5 * (start[k, part, :] * wets[k + 1] + section(own, k))

        dispatch(1, g)

        @pl.when(jnp.logical_not(has_hi))
        def _():
            fold(1, g)

        return carry

    lax.fori_loop(0, chunks, step, 0)

    def last(g, carry):
        receive(1, g)
        part = part_of(g)
        others = {}
        for low, mains, ends in ((-HALO, lo, pack_lo), (rows, hi, pack_hi)):
            for k, t in enumerate(unpacked(ends[1, g], rest)):
                others[low + k] = jnp.concatenate([mains[1, k, part, :], t], axis=1)
        for k in range(rows):
            value = partial[k, part, :]
            for n, (at, _, j) in enumerate(outer):
                if at == k:
                    value += edge[n] * others[j]
            out_ref[part, k, :] = value[:, :nlon]
        return carry

    lax.fori_loop(0, chunks, last, 0)

    for up, near, _, _ in ways:
        @pl.when(near)
        def _(up=up):
            for c in [unmasked(up)] + flows(up):
                c.wait_send()
            for phase in range(2):
                main(phase, up, None).wait_send()
                ends_copy(phase, up, None).wait_send()

    for phase in range(2):
        passed(phase, len(groups[phase]) - 1)


def shards(group, tracers, currents, column_levels):
    tracer, levels, rows, nlon = tracers.shape
    planes = tracer * levels
    width = -(-(nlon + 2 * WRAP) // LANES) * LANES
    whole = nlon - nlon % LANES
    raw = tracers.reshape(planes, rows, nlon)
    chunks = planes // SUB
    groups = pieces_of(chunks)
    count = len(groups[0]) + len(groups[1])
    ends = sum(map(len, pack_sizes(chunks)))
    lat = lax.axis_size("lat")
    layers = lat // group
    relays = layers > 1 and group > 2 and lat % group == 0
    table = detours(groups, layers) if relays else []
    hbm = pl.BlockSpec(memory_space=pltpu.HBM)
    vmem = pl.BlockSpec(memory_space=pltpu.VMEM)
    dma = pltpu.SemaphoreType.DMA

    def f32(*shape):
        return pltpu.VMEM(shape, jnp.float32)

    def i32(*shape):
        return pltpu.VMEM(shape, jnp.int32)

    pack = f32(2, chunks, SUB // 2, LANES)
    args = [pltpu.with_memory_space_constraint(x, pltpu.HBM) for x in (raw, currents, column_levels)]
    out = pl.pallas_call(
        functools.partial(kernel, nlon, levels, group, groups, table),
        out_shape=jax.ShapeDtypeStruct((planes, rows, nlon), jnp.float32),
        in_specs=[hbm] * 3,
        out_specs=vmem,
        scratch_shapes=[
            f32(planes, rows, nlon),
            f32(*currents.shape),
            i32(*column_levels.shape),
            f32(groups[0][0][1] * SUB, HALO, whole),
            f32(groups[0][0][1] * SUB, HALO, whole),
            f32(rows, planes, width),
            f32(rows, planes, width),
            f32(rows, planes, width),
            f32(2, HALO, planes, whole),
            f32(2, HALO, planes, whole),
            f32(2, HALO, planes, whole),
            pack, pack, pack, pack,
            f32(2, rows, levels, nlon),
            f32(levels, nlon),
            f32(levels, nlon),
            i32(HALO, nlon), i32(HALO, nlon),
            f32(rows, 9, SUB, width),
            f32(6, SUB, width),
            f32(rows + 2, SUB, width),
            f32(2 * HALO, SUB, width),
            dma((len(load_sizes(chunks)),)), dma((2,)), dma((2,)), dma((2,)),
            dma((count,)), dma((count,)), dma((count,)), dma((2,)),
            dma((2,)), dma((2,)), dma((ends,)), dma((ends,)), dma((4,)), dma((4,)), dma((2,)),
        ],
        compiler_params=pltpu.CompilerParams(
            collective_id=0, has_side_effects=True, vmem_limit_bytes=44 * 1024 * 1024
        ),
    )(*args)
    return out.reshape(tracers.shape)


def layer_size(mesh):
    devices = mesh.devices.reshape(-1, mesh.shape["lat"])[0]
    spots = [getattr(d, "coords", None) for d in devices]
    if any(s is None or len(s) < 3 for s in spots):
        return 4
    return sum(s[2] == spots[0][2] for s in spots)


def solution(mesh):
    in_specs = (
        P("member", None, "lat", None),
        P("member", None, "lat", None),
        P(("member", "lat"), None),
    )
    out_specs = P("member", None, "lat", None)
    return jax.shard_map(
        functools.partial(shards, layer_size(mesh)),
        mesh=mesh, in_specs=in_specs, out_specs=out_specs, check_vma=False,
    )
```

```python
import functools

import jax
import jax.numpy as jnp
from jax import lax
from jax.experimental import pallas as pl
from jax.experimental.pallas import tpu as pltpu
from jax.sharding import PartitionSpec as P

LANES = 128
SUB = 8
WRAP = 4
HALO = 2
LEAD = 2, 1
WIDEST = 4
PACK_CUT = 3
AHEAD = 2
KEEP = 2
DIRECT = 0.0
MESH = pl.DeviceIdType.MESH


def wrapped(x, nlon):
    rest = nlon % LANES
    whole = nlon - rest
    tail = jnp.concatenate([x[:, whole:], x[:, : LANES - rest]], axis=1)
    lane = lax.broadcasted_iota(jnp.int32, tail.shape, 1)
    tail = jnp.where(lane >= LANES - WRAP, pltpu.roll(tail, LANES - rest, 1), tail)
    return jnp.concatenate([x[:, :whole], tail], axis=1)


def joined(main, tail, rest):
    lane = lax.broadcasted_iota(jnp.int32, tail.shape, 1)
    west = pltpu.roll(tail, LANES - rest, 1)
    tail = jnp.where(lane < rest, tail, pltpu.roll(main[:, :LANES], rest, 1))
    tail = jnp.where(lane >= LANES - WRAP, west, tail)
    return jnp.concatenate([main, tail], axis=1)


def packed(a, b, rest):
    lane = lax.broadcasted_iota(jnp.int32, a.shape, 1)
    both = jnp.where(lane < rest, a, pltpu.roll(b, rest, 1))
    other = pltpu.roll(pltpu.roll(both, SUB // 2, 0), LANES // 2, 1)
    return jnp.where(lane < LANES // 2, both, other)[: SUB // 2]


def unpacked(half, rest):
    x = jnp.concatenate([half, half], axis=0)
    row = lax.broadcasted_iota(jnp.int32, x.shape, 0)
    x = jnp.where(row < SUB // 2, x, pltpu.roll(x, LANES // 2, 1))
    return x, pltpu.roll(x, LANES - rest, 1)


def face_terms(c, opened):
    c = c * opened * (1.0 / 12.0)
    m = jnp.abs(c)
    return -c - m, 7.0 * c + 3.0 * m, 7.0 * c - 3.0 * m, m - c


def mirrored(tiles, nlon):
    count = len(tiles)
    rest = nlon % LANES
    lane = lax.broadcasted_iota(jnp.int32, tiles[0].shape, 1)
    source = jnp.where(lane < rest, rest - 1 - lane, LANES + rest - 1 - lane)
    turned = [jnp.take_along_axis(t, source, axis=1, mode="promise_in_bounds") for t in tiles]
    return [
        jnp.where(lane < rest, turned[(count - 1 - q) % count], turned[(count - 2 - q) % count])
        for q in range(count)
    ]


def growing(n, step):
    sizes = []
    while sum(sizes) < n:
        sizes.append(min(step, n - sum(sizes)))
        step = min(step + 1, WIDEST)
    return sizes


def spans_of(sizes):
    return [(sum(sizes[:i]), n) for i, n in enumerate(sizes)]


def load_sizes(chunks):
    rest = chunks - AHEAD
    return [AHEAD, rest // 3, rest - rest // 3]


def pack_sizes(chunks):
    early = [PACK_CUT]
    while sum(early) < chunks:
        early.append(min(PACK_CUT + 1, chunks - sum(early)))
    return [early, [chunks - PACK_CUT, PACK_CUT]]


def pieces_of(chunks):
    sizes = [AHEAD, 1] + growing(chunks - AHEAD - 3, WIDEST) + [1, 1]
    early = [(at, n, 0, HALO) for at, n in spans_of(sizes)]
    at, n, _, _ = early.pop()
    early += [(at, n, k, 1) for k in range(HALO)]
    late = [(at, n, 0, HALO) for at, n in spans_of(growing(chunks, 1)[::-1])]
    return [early, late]


def subsets(items):
    best = {0: []}
    for size, name in items:
        for total, chosen in list(best.items()):
            best.setdefault(total + size, chosen + [name])
    return best


def detours(groups, layers):
    size = {(p, i): n * k / HALO for p in range(2) for i, (_, n, _, k) in enumerate(groups[p])}
    names = list(size)[1:-KEEP]
    choices = [subsets([(size[n], n) for n in names if n[0] == phase]) for phase in range(2)]
    result = []
    for share in range(layers):
        goal = (sum(size.values()) + DIRECT) * share / layers
        _, one, two = min(
            ((abs(one + two - goal), abs(one - goal / 2)), one, two)
            for one in choices[0] for two in choices[1]
        )
        result.append(choices[0][one] + choices[1][two] if share else [])
    return result


def kernel(
    nlon, levels, group, groups, table, raw_hbm, flow_hbm, lev_hbm, out_ref,
    raw, raw_flow, lev_ref, raw_lo, raw_hi, start, first, partial, lo, hi, relay, pack_up, pack_dn, pack_lo, pack_hi,
    flow, v_lo, v_hi, lev_lo, lev_hi, coef, edge, wets, halo,
    load, aux_load, send_up, send_dn, recv_lo, recv_hi, relay_in, relay_out,
    psend_up, psend_dn, precv_lo, precv_hi, fsend, frecv, send_raw,
):
    lat = lax.axis_size("lat")
    me = lax.axis_index("lat")
    rows, planes, width = start.shape
    rest = nlon % LANES
    whole = nlon - rest
    chunks = planes // SUB
    loads = spans_of(load_sizes(chunks))
    offset = [0, len(groups[0])]
    packs = [spans_of(x) for x in pack_sizes(chunks)]
    first_pack = [0, len(packs[0])]
    layers = lat // group
    layer = me // group
    place = me % group
    relays = bool(table)
    has_lo = me > 0
    has_hi = me < lat - 1
    is_first = place == 0
    is_last = place == group - 1
    barrier = pltpu.get_barrier_semaphore()

    pairs = [(has_lo, -1), (has_hi, 1)]
    if relays:
        pairs += [
            (is_first, group - 1),
            (is_last, 1 - group),
            ((is_first | is_last) & (layer < layers - 1), group),
            ((is_first | is_last) & (layer > 0), -group),
        ]

    def part_of(g):
        return pl.ds(pl.multiple_of(g * SUB, SUB), SUB)

    def loading(i):
        at, n = loads[i]
        part = pl.ds(at * SUB, n * SUB)
        return pltpu.make_async_copy(raw_hbm.at[part], raw.at[part], load.at[i])

    lev_load = pltpu.make_async_copy(lev_hbm, lev_ref, aux_load.at[0])
    flow_load = pltpu.make_async_copy(flow_hbm, raw_flow, aux_load.at[1])
    for near, by in pairs:
        @pl.when(near)
        def _(by=by):
            pl.semaphore_signal(barrier, inc=1, device_id={"lat": me + by}, device_id_type=MESH)

    lev_load.start()
    loading(0).start()
    flow_load.start()

    for i in range(1, len(loads)):
        loading(i).start()

    def remote(src, dst, s, r, by):
        return pltpu.make_async_remote_copy(
            src_ref=src, dst_ref=dst, send_sem=s, recv_sem=r,
            device_id={"lat": me + by}, device_id_type=MESH,
        )

    def flows(up):
        n = 0 if up else 2
        k = rows - 1 if up else 0
        levs = lev_hbm.at[pl.ds(rows - HALO if up else 0, HALO)]
        pieces = [(flow_hbm.at[1, :, k], v_lo if up else v_hi), (levs, lev_lo if up else lev_hi)]
        by = 1 if up else -1
        return [
            remote(src, dst, fsend.at[n + i], frecv.at[n + i], by)
            for i, (src, dst) in enumerate(pieces)
        ]

    def unmasked(up):
        n = groups[0][0][1] * SUB
        src = raw_hbm.at[pl.ds(0, n), pl.ds(rows - HALO if up else 0, HALO), pl.ds(0, whole)]
        s, r = (send_raw.at[0], recv_lo.at[0]) if up else (send_raw.at[1], recv_hi.at[0])
        return remote(src, raw_lo if up else raw_hi, s, r, 1 if up else -1)

    def main(phase, up, i, via=False):
        skip = 0 if phase else groups[0][0][1]
        at, n, k, count = (skip, chunks - skip, 0, HALO) if i is None else groups[phase][i]
        part = pl.ds(at * SUB, n * SUB)
        own = first if phase else start
        src = own.at[pl.ds(k + (rows - HALO if up else 0), count), part, pl.ds(0, whole)]
        s = (send_up if up else send_dn).at[phase]
        r = offset[phase] + (i or 0)
        if via:
            by = 1 - group if up else group - 1
            return remote(src, relay.at[phase, pl.ds(k, count), part], s, relay_in.at[r], by)
        dst = (lo if up else hi).at[phase, pl.ds(k, count), part]
        return remote(src, dst, s, (recv_lo if up else recv_hi).at[r], 1 if up else -1)

    def ends_copy(phase, up, i):
        at, n = (0, chunks) if i is None else packs[phase][i]
        part = pl.ds(at, n)
        i = first_pack[phase] + (i or 0)
        if up:
            return remote(pack_up.at[phase, part], pack_lo.at[phase, part],
                          psend_up.at[phase], precv_lo.at[i], 1)
        return remote(pack_dn.at[phase, part], pack_hi.at[phase, part],
                      psend_dn.at[phase], precv_hi.at[i], -1)

    def forward(phase, up, i):
        at, n, k, count = groups[phase][i]
        part = pl.ds(at * SUB, n * SUB)
        piece = pl.ds(k, count)
        dst = (lo if up else hi).at[phase, piece, part]
        r = (recv_lo if up else recv_hi).at[offset[phase] + i]
        return remote(relay.at[phase, piece, part], dst, relay_out.at[phase], r,
                      group if up else -group)

    def bent(phase, i, share):
        result = False
        for value, chosen in enumerate(table):
            if (phase, i) in chosen:
                result = result | (share == value)
        return result

    names = [(p, i) for p in range(2) for i in range(len(groups[p]))]
    bent_up = {name: bent(*name, layers - 1 - layer) for name in names}
    bent_dn = {name: bent(*name, layer) for name in names}
    ways = ((True, has_hi, is_last, bent_up), (False, has_lo, is_first, bent_dn))
    duties = ((True, is_first, bent_up), (False, is_last, bent_dn))

    def send(phase, i):
        for up, near, end, flags in ways:
            flag = flags[phase, i]
            if flag is False:
                @pl.when(near)
                def _(up=up):
                    main(phase, up, i).start()
            else:
                by_relay = near & end & flag

                @pl.when(by_relay)
                def _(up=up):
                    main(phase, up, i, True).start()

                @pl.when(near & jnp.logical_not(by_relay))
                def _(up=up):
                    main(phase, up, i).start()

    def send_ends(phase, i):
        for up, near, _, _ in ways:
            @pl.when(near)
            def _(up=up):
                ends_copy(phase, up, i).start()

    def pass_on(phase, i):
        if i:
            passed(phase, i - 1)
        for up, end, flags in duties:
            flag = flags[phase, i]
            if flag is not False:
                @pl.when(end & flag)
                def _(up=up):
                    main(phase, up, i, True).wait_recv()
                    forward(phase, up, i).start()

    def passed(phase, i):
        for up, end, flags in duties:
            flag = flags[phase, i]
            if flag is not False:
                @pl.when(end & flag)
                def _(up=up):
                    forward(phase, up, i).wait_send()

    def arrived(copy, phase, i):
        for up, near in ((True, has_lo), (False, has_hi)):
            @pl.when(near)
            def _(up=up):
                copy(phase, up, i).wait_recv()

    def receive(phase, g):
        for i, (at, _, _, _) in enumerate(groups[phase]):
            @pl.when(g == at)
            def _(i=i):
                if i == 0:
                    for j in range(min(LEAD[phase], len(groups[phase]))):
                        pass_on(phase, j)
                if i + LEAD[phase] < len(groups[phase]):
                    pass_on(phase, i + LEAD[phase])
                arrived(main if phase or i else lambda phase, up, i: unmasked(up), phase, i)

        for i, (at, _) in enumerate(packs[phase]):
            @pl.when(g == at)
            def _(i=i):
                arrived(ends_copy, phase, i)

    def dispatch(phase, g):
        for i, (at, n, _, _) in enumerate(groups[phase]):
            if phase or i:
                @pl.when(g == at + n - 1)
                def _(i=i):
                    send(phase, i)

        for i, (at, n) in enumerate(packs[phase]):
            @pl.when(g == at + n - 1)
            def _(i=i):
                send_ends(phase, i)

    pl.semaphore_wait(barrier, sum(jnp.where(near, 1, 0) for near, _ in pairs))

    for up, near, _, _ in ways:
        @pl.when(near)
        def _(up=up):
            unmasked(up).start()
            for c in flows(up):
                c.start()

    ranks = lax.rem(lax.broadcasted_iota(jnp.int32, (SUB, nlon), 0), levels)

    def wet_of(row):
        lev = jnp.broadcast_to(row, (SUB, nlon))
        return wrapped(jnp.where(ranks < lev, 1.0, 0.0), nlon)

    lev_load.wait()
    for k in range(rows):
        wets[k + 1] = wet_of(lev_ref[k : k + 1, :])

    def put_packs(phase, g, tail):
        pack_up[phase, g] = packed(tail(rows - 2), tail(rows - 1), rest)
        pack_dn[phase, g] = packed(tail(0), tail(1), rest)

    def reorder(g):
        part = part_of(g)
        ends = []
        for k in range(rows):
            x = wrapped(raw[part, k, :], nlon) * wets[k + 1]
            start[k, part, :] = x
            ends.append(x[:, whole:])
        put_packs(0, g, lambda k: ends[k])

    loading(0).wait()
    reorder(0)
    flow_load.wait()
    for k in range(rows):
        for which in range(2):
            flow[which, k] = raw_flow[which, :, k, :]

    def begin(g, carry):
        for i, (at, _) in enumerate(loads):
            if i:
                @pl.when(g == at)
                def _(i=i):
                    loading(i).wait()

        reorder(g)

        @pl.when(g > 1)
        def _():
            dispatch(0, g - 1)

        return carry

    lax.fori_loop(1, chunks, begin, 0)

    spans = [(q * LANES, min(LANES, nlon - q * LANES)) for q in range(width // LANES)]

    def tiles_of(x):
        return [x[:, q * LANES : (q + 1) * LANES] for q in range(width // LANES)]

    def fold(phase, g):
        part = part_of(g)
        own = first if phase else start
        ends = []
        for k in range(HALO):
            tiles = mirrored(tiles_of(own[rows - 1 - k, part, :]), nlon)
            for (at, n), t in zip(spans[:-1], tiles[:-1]):
                hi[phase, k, part, at : at + n] = t
            ends.append(tiles[-1])
        pack_hi[phase, g] = packed(*ends, rest)

    @pl.when(jnp.logical_not(has_lo))
    def _():
        v_lo[...] = jnp.zeros_like(v_lo)
        lev_lo[...] = jnp.zeros_like(lev_lo)
        lo[...] = jnp.zeros_like(lo)
        pack_lo[...] = jnp.zeros_like(pack_lo)

    @pl.when(jnp.logical_not(has_hi))
    def _():
        lev = jnp.broadcast_to(lev_ref[rows - 1 : rows, :].astype(jnp.float32), (SUB - levels, nlon))
        x = jnp.concatenate([flow[1, rows - 1], lev], axis=0)
        x = jnp.concatenate([x, jnp.zeros((SUB, width - nlon), jnp.float32)], axis=1)
        for (at, n), t in zip(spans, mirrored(tiles_of(x), nlon)):
            v_hi[:, at : at + n] = -t[:levels, :n]
            lev_hi[0:1, at : at + n] = (t[levels : levels + 1, :n] + 0.5).astype(jnp.int32)

        def fold_start(g, carry):
            fold(0, g)
            return carry

        lax.fori_loop(0, chunks, fold_start, 0)

    @pl.when(has_lo)
    def _():
        for c in flows(True):
            c.wait_recv()

    @pl.when(has_hi)
    def _():
        for c in flows(False):
            c.wait_recv()

    def shift(x, by):
        return pltpu.roll(x, (-by) % width, 1)

    wets[0] = wet_of(lev_lo[HALO - 1 : HALO, :])
    wets[rows + 1] = wet_of(lev_hi[0:1, :])

    def spread(x):
        return wrapped(jnp.concatenate([x] * (SUB // levels), axis=0), nlon)

    def v_row(j):
        if j < 0:
            return spread(v_lo[...])
        if j >= rows:
            return spread(v_hi[...])
        return spread(flow[1, j])

    def north_face(j):
        return face_terms(0.5 * (v_row(j) + v_row(j + 1)), wets[j + 1] * wets[j + 2])

    dispatch(0, chunks - 1)

    below = north_face(-1)
    for k in range(rows):
        wet = wets[k + 1]
        u = spread(flow[0, k])
        ea, eb, ed, ee = face_terms(0.5 * (u + shift(u, 1)), wet * shift(wet, 1))
        above = north_face(k)
        coef[k, 0] = wet * shift(ea, -1)
        coef[k, 1] = wet * (shift(eb, -1) - ea)
        coef[k, 2] = wet * (shift(ee, -1) - ed)
        coef[k, 3] = wet * -ee
        coef[k, 4] = wet * below[0]
        coef[k, 5] = wet * (below[1] - above[0])
        coef[k, 6] = wet * (below[3] - above[2])
        coef[k, 7] = wet * -above[3]
        coef[k, 8] = wet * (1.0 - eb + shift(ed, -1) - above[1] + below[2])
        below = above

    outer = [
        (k, 4 + i, k + d)
        for k in range(rows)
        for i, d in enumerate((-2, -1, 1, 2))
        if not 0 <= k + d < rows
    ]
    for n, (k, i, _) in enumerate(outer):
        edge[n] = 0.5 * coef[k, i]

    def section(get, k):
        f = get(k)
        total = coef[k, 8] * f
        total += coef[k, 0] * shift(f, -2)
        total += coef[k, 1] * shift(f, -1)
        total += coef[k, 2] * shift(f, 1)
        total += coef[k, 3] * shift(f, 2)
        for i, d in enumerate((-2, -1, 1, 2)):
            other = get(k + d)
            if other is not None:
                total += coef[k, 4 + i] * other
        return total

    def mask_first(g):
        part = part_of(g)
        for near, source, levs, mains in ((has_lo, raw_lo, lev_lo, lo), (has_hi, raw_hi, lev_hi, hi)):
            @pl.when(near)
            def _(source=source, levs=levs, mains=mains):
                for k in range(HALO):
                    wet = jnp.where(ranks < jnp.broadcast_to(levs[k : k + 1, :], (SUB, nlon)), 1.0, 0.0)
                    mains[0, k, part, :] = source[part, k, :] * wet[:, :whole]

    def step(g, carry):
        receive(0, g)

        @pl.when(g < groups[0][0][1])
        def _():
            mask_first(g)

        part = part_of(g)
        for low, mains, ends in ((0, lo, pack_lo), (HALO, hi, pack_hi)):
            for k, t in enumerate(unpacked(ends[0, g], rest)):
                halo[low + k] = joined(mains[0, k, part, :], t, rest)

        def field(j):
            if j < 0:
                return halo[j + HALO]
            if j >= rows:
                return halo[j - rows + HALO]
            return start[j, part, :]

        for k in range(rows):
            first[k, part, :] = section(field, k)
        put_packs(1, g, lambda k: first[k, part, whole:])

        def own(j):
            return first[j, part, :] if 0 <= j < rows else None

        for k in range(rows):
            partial[k, part, :] = 0.5 * (start[k, part, :] * wets[k + 1] + section(own, k))

        dispatch(1, g)

        @pl.when(jnp.logical_not(has_hi))
        def _():
            fold(1, g)

        return carry

    lax.fori_loop(0, chunks, step, 0)

    def last(g, carry):
        receive(1, g)
        part = part_of(g)
        others = {}
        for low, mains, ends in ((-HALO, lo, pack_lo), (rows, hi, pack_hi)):
            for k, t in enumerate(unpacked(ends[1, g], rest)):
                others[low + k] = jnp.concatenate([mains[1, k, part, :], t], axis=1)
        for k in range(rows):
            value = partial[k, part, :]
            for n, (at, _, j) in enumerate(outer):
                if at == k:
                    value += edge[n] * others[j]
            out_ref[part, k, :] = value[:, :nlon]
        return carry

    lax.fori_loop(0, chunks, last, 0)

    for up, near, _, _ in ways:
        @pl.when(near)
        def _(up=up):
            for c in [unmasked(up)] + flows(up):
                c.wait_send()
            for phase in range(2):
                main(phase, up, None).wait_send()
                ends_copy(phase, up, None).wait_send()

    for phase in range(2):
        passed(phase, len(groups[phase]) - 1)


def shards(group, tracers, currents, column_levels):
    tracer, levels, rows, nlon = tracers.shape
    planes = tracer * levels
    width = -(-(nlon + 2 * WRAP) // LANES) * LANES
    whole = nlon - nlon % LANES
    raw = tracers.reshape(planes, rows, nlon)
    chunks = planes // SUB
    groups = pieces_of(chunks)
    count = len(groups[0]) + len(groups[1])
    ends = sum(map(len, pack_sizes(chunks)))
    lat = lax.axis_size("lat")
    layers = lat // group
    relays = layers > 1 and group > 2 and lat % group == 0
    table = detours(groups, layers) if relays else []
    hbm = pl.BlockSpec(memory_space=pltpu.HBM)
    vmem = pl.BlockSpec(memory_space=pltpu.VMEM)
    dma = pltpu.SemaphoreType.DMA

    def f32(*shape):
        return pltpu.VMEM(shape, jnp.float32)

    def i32(*shape):
        return pltpu.VMEM(shape, jnp.int32)

    pack = f32(2, chunks, SUB // 2, LANES)
    args = [pltpu.with_memory_space_constraint(x, pltpu.HBM) for x in (raw, currents, column_levels)]
    out = pl.pallas_call(
        functools.partial(kernel, nlon, levels, group, groups, table),
        out_shape=jax.ShapeDtypeStruct((planes, rows, nlon), jnp.float32),
        in_specs=[hbm] * 3,
        out_specs=vmem,
        scratch_shapes=[
            f32(planes, rows, nlon),
            f32(*currents.shape),
            i32(*column_levels.shape),
            f32(groups[0][0][1] * SUB, HALO, whole),
            f32(groups[0][0][1] * SUB, HALO, whole),
            f32(rows, planes, width),
            f32(rows, planes, width),
            f32(rows, planes, width),
            f32(2, HALO, planes, whole),
            f32(2, HALO, planes, whole),
            f32(2, HALO, planes, whole),
            pack, pack, pack, pack,
            f32(2, rows, levels, nlon),
            f32(levels, nlon),
            f32(levels, nlon),
            i32(HALO, nlon), i32(HALO, nlon),
            f32(rows, 9, SUB, width),
            f32(6, SUB, width),
            f32(rows + 2, SUB, width),
            f32(2 * HALO, SUB, width),
            dma((len(load_sizes(chunks)),)), dma((2,)), dma((2,)), dma((2,)),
            dma((count,)), dma((count,)), dma((count,)), dma((2,)),
            dma((2,)), dma((2,)), dma((ends,)), dma((ends,)), dma((4,)), dma((4,)), dma((2,)),
        ],
        compiler_params=pltpu.CompilerParams(
            collective_id=0, has_side_effects=True, vmem_limit_bytes=44 * 1024 * 1024
        ),
    )(*args)
    return out.reshape(tracers.shape)


def layer_size(mesh):
    devices = mesh.devices.reshape(-1, mesh.shape["lat"])[0]
    spots = [getattr(d, "coords", None) for d in devices]
    if any(s is None or len(s) < 3 for s in spots):
        return 4
    return sum(s[2] == spots[0][2] for s in spots)


def solution(mesh):
    in_specs = (
        P("member", None, "lat", None),
        P("member", None, "lat", None),
        P(("member", "lat"), None),
    )
    out_specs = P("member", None, "lat", None)
    return jax.shard_map(
        functools.partial(shards, layer_size(mesh)),
        mesh=mesh, in_specs=in_specs, out_specs=out_specs, check_vma=False,
    )
```
